8 devices in a mesh: dp: 1 (over z), fsdp: 8 (over y, x, core).
Axes of the slice: x: 2, y: 2, z: 1, core: 2. Of those that a mesh axis runs over, the one named last changes fastest.
Arguments:
- hidden_in: bfloat16 [8, 192, 2048], P(('dp', 'fsdp'))
- lengths: int32 [8], P(('dp', 'fsdp'))
- ln_attn_g: float32 [2, 2048], P(None, 'fsdp')
- ln_attn_b: float32 [2, 2048], P(None, 'fsdp')
- ln_mlp_g: float32 [2, 2048], P(None, 'fsdp')
- ln_mlp_b: float32 [2, 2048], P(None, 'fsdp')
- w_qkv: bfloat16 [2, 2048, 4, 4, 256], P(None, 'fsdp')
- w_out: bfloat16 [2, 2048, 2048], P(None, 'fsdp')
- w_up: bfloat16 [2, 2048, 8192], P(None, 'fsdp')
- w_down: bfloat16 [2, 8192, 2048], P(None, 'fsdp')
Outputs:
- output 1: bfloat16 [8, 192, 2048], P(('dp', 'fsdp'))
- output 2: bfloat16 [2, 8, 4, 192, 256], P(None, ('dp', 'fsdp'))
- output 3: bfloat16 [2, 8, 4, 192, 256], P(None, ('dp', 'fsdp'))
All inputs are finite; a program needn't handle non-finite values.
Results may differ from the reference program's by a relative error of at most 0.0100703.
Values are sent between devices in bfloat16 or wider.
A program may use at most 1 GiB of HBM per device.

```python
import jax
import jax.numpy as jnp
from jax import lax

SEQ_COUNT = 8
SEQ_LEN = 192
D_MODEL = 2048
N_HEADS = 8
KV_HEADS = 4
HEAD_DIM = 256
FF_DIM = 8192
NUM_LAYERS = 2
GROUP_HEADS = N_HEADS // KV_HEADS
LN_EPS = 1e-5
ROPE_BASE = 10000.0


def setup_inputs(seed: int = 0, part: int = 0) -> dict:
    base_key = jax.random.key(seed)
    part_key = jax.random.fold_in(base_key, part)
    key_x, key_len = jax.random.split(part_key, 2)
    weight_keys = jax.random.split(base_key, 8)
    attn_width = N_HEADS * HEAD_DIM
    shape_vec = (NUM_LAYERS, D_MODEL)
    qkv_shape = (NUM_LAYERS, D_MODEL, KV_HEADS, GROUP_HEADS + 2, HEAD_DIM)
    hidden = jax.random.normal(key_x, (SEQ_COUNT, SEQ_LEN, D_MODEL), jnp.float32)
    lengths = jax.random.randint(key_len, (SEQ_COUNT,), 1, SEQ_LEN + 1, dtype=jnp.int32)
    lengths = lengths.at[0].set(SEQ_LEN)
    return {
        "hidden_in": hidden.astype(jnp.bfloat16),
        "lengths": lengths,
        "ln_attn_g": 1.0 + 0.3 * jax.random.normal(weight_keys[0], shape_vec, jnp.float32),
        "ln_attn_b": 0.3 * jax.random.normal(weight_keys[1], shape_vec, jnp.float32),
        "ln_mlp_g": 1.0 + 0.3 * jax.random.normal(weight_keys[2], shape_vec, jnp.float32),
        "ln_mlp_b": 0.3 * jax.random.normal(weight_keys[3], shape_vec, jnp.float32),
        "w_qkv": (jax.random.normal(weight_keys[4], qkv_shape, jnp.float32) * D_MODEL ** -0.5).astype(jnp.bfloat16),
        "w_out": (jax.random.normal(weight_keys[5], (NUM_LAYERS, attn_width, D_MODEL), jnp.float32) * attn_width ** -0.5).astype(jnp.bfloat16),
        "w_up": (jax.random.normal(weight_keys[6], (NUM_LAYERS, D_MODEL, FF_DIM), jnp.float32) * D_MODEL ** -0.5).astype(jnp.bfloat16),
        "w_down": (jax.random.normal(weight_keys[7], (NUM_LAYERS, FF_DIM, D_MODEL), jnp.float32) * FF_DIM ** -0.5).astype(jnp.bfloat16),
    }


def layer_norm(hidden, gain_vec, bias_vec):
    hidden_f = hidden.astype(jnp.float32)
    row_mean = jnp.mean(hidden_f, axis=-1, keepdims=True)
    centered = hidden_f - row_mean
    variance = jnp.mean(centered * centered, axis=-1, keepdims=True)
    return (centered * lax.rsqrt(variance + LN_EPS) * gain_vec + bias_vec).astype(jnp.bfloat16)


def rope_tables(seq_len, head_dim):
    half_dim = head_dim // 2
    inv_freq = ROPE_BASE ** (-2.0 * jnp.arange(half_dim, dtype=jnp.float32) / head_dim)
    angles = jnp.arange(seq_len, dtype=jnp.float32)[:, None] * inv_freq[None, :]
    cos_half = jnp.cos(angles)
    sin_half = jnp.sin(angles)
    return jnp.concatenate([cos_half, cos_half], axis=-1), jnp.concatenate([sin_half, sin_half], axis=-1)


def rotary(values, cos_full, sin_full):
    vals_f = values.astype(jnp.float32)
    half_dim = vals_f.shape[-1] // 2
    rotated = jnp.concatenate([-vals_f[..., half_dim:], vals_f[..., :half_dim]], axis=-1)
    return (vals_f * cos_full + rotated * sin_full).astype(jnp.bfloat16)


def decoder_layer(hidden, params, length):
    gain_a, bias_a, gain_m, bias_m, w_qkv, w_out, w_up, w_down = params
    seq_len = hidden.shape[0]
    attn_in = layer_norm(hidden, gain_a, bias_a)
    mlp_in = layer_norm(hidden, gain_m, bias_m)
    qkv_proj = jnp.einsum("td,dkgh->tkgh", attn_in.astype(jnp.float32), w_qkv.astype(jnp.float32)).astype(jnp.bfloat16)
    cos_full, sin_full = rope_tables(seq_len, HEAD_DIM)
    queries = rotary(qkv_proj[:, :, :GROUP_HEADS], cos_full[:, None, None, :], sin_full[:, None, None, :])
    key_rot = rotary(qkv_proj[:, :, GROUP_HEADS], cos_full[:, None, :], sin_full[:, None, :])
    values = qkv_proj[:, :, GROUP_HEADS + 1]
    scores = jnp.einsum("qkgh,skh->kgqs", queries.astype(jnp.float32), key_rot.astype(jnp.float32)) * HEAD_DIM ** -0.5
    positions = jnp.arange(seq_len)
    allowed = (positions[None, :] <= positions[:, None]) & (positions[None, :] < length)
    attn_prob = jax.nn.softmax(jnp.where(allowed, scores, -1e30), axis=-1).astype(jnp.bfloat16)
    context = jnp.einsum("kgqs,skh->qkgh", attn_prob.astype(jnp.float32), values.astype(jnp.float32)).astype(jnp.bfloat16)
    context = context.reshape(seq_len, N_HEADS * HEAD_DIM)
    attn_out = jnp.dot(context, w_out, preferred_element_type=jnp.float32)
    hidden_mlp = jax.nn.gelu(jnp.dot(mlp_in, w_up, preferred_element_type=jnp.float32), approximate=False).astype(jnp.bfloat16)
    mlp_out = jnp.dot(hidden_mlp, w_down, preferred_element_type=jnp.float32)
    new_hidden = (hidden.astype(jnp.float32) + attn_out + mlp_out).astype(jnp.bfloat16)
    return new_hidden, jnp.swapaxes(key_rot, 0, 1), jnp.swapaxes(values, 0, 1)


def reference(hidden_in, lengths, ln_attn_g, ln_attn_b, ln_mlp_g, ln_mlp_b, w_qkv, w_out, w_up, w_down):
    layer_params = (ln_attn_g, ln_attn_b, ln_mlp_g, ln_mlp_b, w_qkv, w_out, w_up, w_down)

    def one_sequence(seq_item):
        seq_x, seq_length = seq_item

        def layer_step(hidden, params):
            new_hidden, key_cache, value_cache = decoder_layer(hidden, params, seq_length)
            return new_hidden, (key_cache, value_cache)

        final_h, caches = lax.scan(layer_step, seq_x, layer_params)
        return final_h, caches[0], caches[1]

    hidden_out, key_caches, value_caches = lax.map(one_sequence, (hidden_in, lengths))
    return hidden_out, jnp.swapaxes(key_caches, 0, 1), jnp.swapaxes(value_caches, 0, 1)
```

```python
import jax
import jax.numpy as jnp
import numpy as np
from jax import lax
from jax.experimental import pallas as pl
from jax.experimental.pallas import tpu as pltpu
from jax.sharding import PartitionSpec as P

MESH = pl.DeviceIdType.MESH
LN_EPS = 1e-5
ROPE_BASE = 10000.0
T = 192
D = 2048
HD = 256
ROWS = 256
QC = 1024
FC = 2048
DR = 1024
CH = 16
TN = 256
F32 = jnp.float32
BF16 = jnp.bfloat16
PACK, QKV0, UP0, QKV1, UP1 = range(5)


def kernel(pack, h_in, wqkv, wout, wup, wdown, cos_ref, sin_ref,
           h_out, kc, vc,
           packg, wq, wu, wo, wd, hg, part, rsb, nb, qkv, ctx, kr, vr, mid,
           ici_s, ici_r, d2d_s, d2d_r, loc, own_s, own_r, own_l,
           h_s, h_r, h_l, rs_s, rs_r, kv_s, kv_r, kv_l, out_l):
    me = lax.axis_index("fsdp")
    core = me % 2
    chip = me // 2
    partner = chip * 2 + (1 - core)

    def chip_at(s):
        return ((chip // 2 + s // 2) % 2) * 2 + (chip % 2 + s % 2) % 2

    def peer(s):
        return chip_at(s) * 2 + core

    def remote(src, dst, send, recv, device):
        return pltpu.make_async_remote_copy(
            src_ref=src, dst_ref=dst, send_sem=send, recv_sem=recv,
            device_id={"fsdp": device}, device_id_type=MESH)

    def cols(c, width):
        return pl.ds(pl.multiple_of(c * width, width), width)

    def source(kind, c):
        if kind == PACK:
            return pack
        if kind in (QKV0, QKV1):
            return wqkv.at[int(kind == QKV1), :, cols(c, QC)]
        return wup.at[int(kind == UP1), :, cols(c, FC)]

    def landing(kind, row):
        if kind == PACK:
            return packg.at[:, cols(row, ROWS)]
        if kind in (QKV0, QKV1):
            return wq.at[int(kind == QKV1), cols(row, ROWS), :]
        return wu.at[int(kind == UP1), cols(row, ROWS), :]

    def ici(kind, s):
        return remote(source(kind, chip_at(s)), landing(kind, me), ici_s.at[kind, s], ici_r.at[kind, s], peer(s))

    def ici_in(kind, s):
        return remote(source(kind, chip), landing(kind, peer(s)), ici_s.at[kind, s], ici_r.at[kind, s], peer(s))

    def d2d(kind, s):
        src = source(kind, chip) if s == 0 else landing(kind, peer(s))
        row = me if s == 0 else peer(s)
        return remote(src, landing(kind, row), d2d_s.at[kind, s], d2d_r.at[kind, s], partner)

    def d2d_in(kind, s):
        row = chip_at(s) * 2 + (1 - core)
        return remote(landing(kind, row), landing(kind, row), d2d_s.at[kind, s], d2d_r.at[kind, s], partner)

    def local(kind):
        return pltpu.make_async_copy(source(kind, chip), landing(kind, me), loc.at[kind])

    def own_refs(layer, which, core_index):
        if which == 0:
            return wout.at[layer], wo.at[layer, cols(core_index, ROWS), :]
        return wdown.at[layer], wd.at[layer, cols(core_index, DR), :]

    def own_remote(layer, which, core_index):
        src, dst = own_refs(layer, which, core_index)
        return remote(src, dst, own_s.at[layer, which], own_r.at[layer, which], partner)

    def own_local(layer, which):
        src, dst = own_refs(layer, which, core)
        return pltpu.make_async_copy(src, dst, own_l.at[layer, which])

    def send_block(kind):
        for s in (3, 1, 2):
            ici(kind, s).start()

    def own_block(kind):
        local(kind).start()
        d2d(kind, 0).start()

    def own_rows(layer):
        for which in range(2):
            own_local(layer, which).start()
            own_remote(layer, which, core).start()

    def relay_block(kind):
        for s in (3, 1, 2):
            ici_in(kind, s).wait_recv()
            d2d(kind, s).start()

    def block_ready(kind):
        local(kind).wait()
        for s in range(4):
            d2d_in(kind, s).wait_recv()

    def own_ready(layer):
        for which in range(2):
            own_local(layer, which).wait()
            own_remote(layer, which, 1 - core).wait_recv()

    def h_copy(layer, s):
        src = h_in if layer == 0 else hg.at[chip]
        return remote(src, hg.at[chip], h_s.at[layer, s], h_r.at[layer, s], peer(s))

    def h_copy_in(layer, s):
        return remote(hg.at[chip_at(s)], hg.at[chip_at(s)], h_s.at[layer, s], h_r.at[layer, s], peer(s))

    def rs_copy(layer, s):
        return remote(part.at[chip_at(s)], rsb.at[s - 1], rs_s.at[layer, s], rs_r.at[layer, s], peer(s))

    def kv_copy(layer, which, s):
        src = (kr, vr)[which].at[chip_at(s)]
        dst = (kc, vc)[which].at[layer, chip]
        return remote(src, dst, kv_s.at[layer, which, s], kv_r.at[layer, which, s], peer(s))

    def kv_copy_in(layer, which, s):
        dst = (kc, vc)[which].at[layer, chip_at(s)]
        return remote(dst, dst, kv_s.at[layer, which, s], kv_r.at[layer, which, s], peer(s))

    def kv_local(layer, which):
        return pltpu.make_async_copy((kr, vr)[which].at[chip], (kc, vc)[which].at[layer, chip], kv_l.at[layer, which])

    def kv_send(layer):
        for which in range(2):
            kv_local(layer, which).start()
            for s in (3, 1, 2):
                kv_copy(layer, which, s).start()

    def kv_sent(layer):
        for which in range(2):
            kv_local(layer, which).wait()
            for s in (3, 1, 2):
                kv_copy(layer, which, s).wait_send()

    def norm(j, gain_row):
        gain = packg[gain_row:gain_row + 1, :]
        bias = packg[gain_row + 2:gain_row + 3, :]

        def step(i, carry):
            rows = pl.ds(pl.multiple_of(i * CH, CH), CH)
            x = hg[j, rows, :].astype(F32)
            mean = jnp.sum(x, axis=-1, keepdims=True) * (1.0 / D)
            x = x - mean
            var = jnp.sum(x * x, axis=-1, keepdims=True) * (1.0 / D)
            nb[rows, :] = (x * lax.rsqrt(var + LN_EPS) * gain + bias).astype(BF16)
            return carry

        lax.fori_loop(0, T // CH, step, 0)

    def rope(u):
        u = u.astype(F32)
        lo, hi = u[:, :HD // 2], u[:, HD // 2:]
        cos, sin = cos_ref[...], sin_ref[...]
        return jnp.concatenate([lo * cos - hi * sin, hi * cos + lo * sin], axis=-1).astype(BF16)

    def attention(layer, j):
        norm(j, layer)

        def project(i, carry):
            n = cols(i, TN)
            qkv[:, n] = jnp.dot(nb[...], wq[layer, :, n], preferred_element_type=F32).astype(BF16)
            return carry

        lax.fori_loop(0, QC // TN, project, 0)
        key = rope(qkv[:, 2 * HD:3 * HD])
        kr[j] = key
        vr[j] = qkv[:, 3 * HD:4 * HD]
        length = packg[8:9, pl.ds(pl.multiple_of((j * 2 + core) * ROWS, ROWS), 128)][:, 0:1]
        query_pos = lax.broadcasted_iota(jnp.int32, (T, T), 0)
        key_pos = lax.broadcasted_iota(jnp.int32, (T, T), 1)
        allowed = (key_pos <= query_pos) & (key_pos.astype(F32) < length)
        for head in range(2):
            query = rope(qkv[:, head * HD:(head + 1) * HD])
            scores = lax.dot_general(query, key, (((1,), (1,)), ((), ())), preferred_element_type=F32) * (HD ** -0.5)
            scores = jnp.where(allowed, scores, -1e30)
            expo = jnp.exp(scores - jnp.max(scores, axis=-1, keepdims=True))
            prob = (expo / jnp.sum(expo, axis=-1, keepdims=True)).astype(BF16)
            ctx[j, :, head * HD:(head + 1) * HD] = jnp.dot(prob, vr[j], preferred_element_type=F32).astype(BF16)

    def mlp(layer, j):
        norm(j, 4 + layer)

        def up(i, carry):
            n = cols(i, TN)
            u = jnp.dot(nb[...], wu[layer, :, n], preferred_element_type=F32)
            mid[:, n] = (0.5 * u * (1.0 + lax.erf(u * np.float32(np.sqrt(0.5))))).astype(BF16)
            return carry

        lax.fori_loop(0, FC // TN, up, 0)

        def down(i, carry):
            n = cols(i, TN)
            acc = jnp.dot(mid[...], wd[layer, :, n], preferred_element_type=F32)
            part[j, :, n] = acc + jnp.dot(ctx[j], wo[layer, :, n], preferred_element_type=F32)
            return carry

        lax.fori_loop(0, D // TN, down, 0)

    def residual(layer):
        for s in (3, 1, 2):
            rs_copy(layer, s).wait_recv()

        def step(i, carry):
            rows = pl.ds(pl.multiple_of(i * CH, CH), CH)
            total = hg[chip, rows, :].astype(F32) + part[chip, rows, :]
            total = total + rsb[0, rows, :] + rsb[1, rows, :] + rsb[2, rows, :]
            hg[chip, rows, :] = total.astype(BF16)
            return carry

        lax.fori_loop(0, T // CH, step, 0)

    barrier = pltpu.get_barrier_semaphore()
    for s in (1, 2, 3):
        pl.semaphore_signal(barrier, inc=1, device_id={"fsdp": peer(s)}, device_id_type=MESH)
    pl.semaphore_signal(barrier, inc=1, device_id={"fsdp": partner}, device_id_type=MESH)
    pl.semaphore_wait(barrier, 4)

    send_block(PACK)
    own_block(PACK)
    for s in (3, 1, 2):
        h_copy(0, s).start()
    h_local = pltpu.make_async_copy(h_in, hg.at[chip], h_l.at[0])
    h_local.start()
    send_block(QKV0)
    send_block(UP0)
    own_block(QKV0)
    own_block(UP0)
    own_rows(0)

    relay_block(PACK)
    block_ready(PACK)
    h_local.wait()
    for s in (3, 1, 2):
        h_copy_in(0, s).wait_recv()
    relay_block(QKV0)
    block_ready(QKV0)

    def attend_step(s, carry):
        attention(0, chip_at(s))
        return carry

    lax.fori_loop(0, 4, attend_step, 0)
    kv_send(0)
    send_block(QKV1)
    own_block(QKV1)
    own_block(UP1)
    own_rows(1)
    relay_block(UP0)
    block_ready(UP0)
    own_ready(0)

    def mlp_step(i, carry):
        s = 3 - i
        mlp(0, chip_at(s))

        @pl.when(s > 0)
        def _():
            rs_copy(0, s).start()

        return carry

    lax.fori_loop(0, 4, mlp_step, 0)
    send_block(UP1)
    relay_block(QKV1)
    for s in (3, 1, 2):
        h_copy(0, s).wait_send()
    residual(0)
    for s in (3, 1, 2):
        h_copy(1, s).start()
    relay_block(UP1)
    block_ready(QKV1)
    block_ready(UP1)
    own_ready(1)
    kv_sent(0)
    for s in (3, 1, 2):
        rs_copy(0, s).wait_send()

    def layer_step(i, carry):
        s = (4 - i) % 4

        @pl.when(s > 0)
        def _():
            h_copy_in(1, s).wait_recv()

        attention(1, chip_at(s))
        mlp(1, chip_at(s))

        @pl.when(s > 0)
        def _():
            rs_copy(1, s).start()

        return carry

    lax.fori_loop(0, 4, layer_step, 0)
    kv_send(1)
    for s in (3, 1, 2):
        h_copy(1, s).wait_send()
    residual(1)
    final = pltpu.make_async_copy(hg.at[chip], h_out, out_l.at[0])
    final.start()

    for kind in range(5):
        for s in (3, 1, 2):
            ici(kind, s).wait_send()
        for s in range(4):
            d2d(kind, s).wait_send()
    for layer in range(2):
        for which in range(2):
            own_remote(layer, which, core).wait_send()
    for s in (3, 1, 2):
        rs_copy(1, s).wait_send()
    kv_sent(1)
    for layer in range(2):
        for which in range(2):
            for s in (3, 1, 2):
                kv_copy_in(layer, which, s).wait_recv()
    final.wait()


def rope_tables():
    half = HD // 2
    inv_freq = np.float32(ROPE_BASE) ** (np.float32(-2.0) * np.arange(half, dtype=np.float32) / np.float32(HD))
    angles = np.arange(T, dtype=np.float32)[:, None] * inv_freq.astype(np.float32)[None, :]
    return np.cos(angles).astype(np.float32), np.sin(angles).astype(np.float32)


def solution(mesh):
    batch_spec = P(("dp", "fsdp"))
    weight_spec = P(None, "fsdp")
    cache_spec = P(None, ("dp", "fsdp"))
    vmem = pl.BlockSpec(memory_space=pltpu.VMEM)
    hbm = pl.BlockSpec(memory_space=pl.ANY)
    dma = pltpu.SemaphoreType.DMA

    def per_device(hidden_in, lengths, ln_attn_g, ln_attn_b, ln_mlp_g, ln_mlp_b, w_qkv, w_out, w_up, w_down):
        length_rows = jnp.broadcast_to(lengths.astype(F32)[:, None], (8, ROWS))
        pack = jnp.concatenate([ln_attn_g, ln_attn_b, ln_mlp_g, ln_mlp_b, length_rows], axis=0)
        cos, sin = rope_tables()
        call = pl.pallas_call(
            kernel,
            out_shape=(
                jax.ShapeDtypeStruct((T, D), BF16),
                jax.ShapeDtypeStruct((2, 4, T, HD), BF16),
                jax.ShapeDtypeStruct((2, 4, T, HD), BF16),
            ),
            in_specs=[vmem, hbm, hbm, hbm, hbm, hbm, vmem, vmem],
            out_specs=(hbm, hbm, hbm),
            scratch_shapes=[
                pltpu.VMEM((16, D), F32),
                pltpu.VMEM((2, D, QC), BF16),
                pltpu.VMEM((2, D, FC), BF16),
                pltpu.VMEM((2, 2 * ROWS, D), BF16),
                pltpu.VMEM((2, 2 * DR, D), BF16),
                pltpu.VMEM((4, T, D), BF16),
                pltpu.VMEM((4, T, D), F32),
                pltpu.VMEM((3, T, D), F32),
                pltpu.VMEM((T, D), BF16),
                pltpu.VMEM((T, QC), BF16),
                pltpu.VMEM((4, T, 2 * HD), BF16),
                pltpu.VMEM((4, T, HD), BF16),
                pltpu.VMEM((4, T, HD), BF16),
                pltpu.VMEM((T, FC), BF16),
                dma((5, 4)), dma((5, 4)), dma((5, 4)), dma((5, 4)), dma((5,)),
                dma((2, 2)), dma((2, 2)), dma((2, 2)),
                dma((2, 4)), dma((2, 4)), dma((1,)),
                dma((2, 4)), dma((2, 4)),
                dma((2, 2, 4)), dma((2, 2, 4)), dma((2, 2)), dma((1,)),
            ],
            compiler_params=pltpu.CompilerParams(
                collective_id=0, has_side_effects=True, vmem_limit_bytes=67043328),
            name="decoder_layers",
        )
        h_out, kc, vc = call(pack, hidden_in[0], w_qkv.reshape(2, ROWS, 4 * QC), w_out, w_up, w_down, cos, sin)
        return h_out[None], kc[:, None], vc[:, None]

    return jax.shard_map(per_device, mesh=mesh, in_specs=(batch_spec, batch_spec) + (weight_spec,) * 8, out_specs=(batch_spec, cache_spec, cache_spec), check_vma=False)
```

```python
import jax
import jax.numpy as jnp
import numpy as np
from jax import lax
from jax.experimental import pallas as pl
from jax.experimental.pallas import tpu as pltpu
from jax.sharding import PartitionSpec as P

MESH = pl.DeviceIdType.MESH
LN_EPS = 1e-5
ROPE_BASE = 10000.0
T = 192
D = 2048
HD = 256
ROWS = 256
QC = 1024
FC = 2048
DR = 1024
HALF = D // 2
CH = 16
TN = 256
F32 = jnp.float32
BF16 = jnp.bfloat16
PACK, QKV0, UP0, QKV1, UP1 = range(5)


def kernel(pack, h_in, wqkv, wout, wup, wdown, cos_ref, sin_ref,
           h_out, kc, vc,
           packg, wq, wu, wo, wd, hg, part, rsd, rsb, nb, qkv, ctx, kr, vr, mid,
           ici_s, ici_r, d2d_s, d2d_r, loc, own_s, own_r, own_l,
           h_s, h_r, hf_s, hf_r, h_l, rs_s, rs_r, kv_s, kv_r, kv_l, out_l):
    me = lax.axis_index("fsdp")
    core = me % 2
    chip = me // 2
    partner = chip * 2 + (1 - core)

    def chip_at(s):
        return ((chip // 2 + s // 2) % 2) * 2 + (chip % 2 + s % 2) % 2

    def peer(s):
        return chip_at(s) * 2 + core

    def remote(src, dst, send, recv, device):
        return pltpu.make_async_remote_copy(
            src_ref=src, dst_ref=dst, send_sem=send, recv_sem=recv,
            device_id={"fsdp": device}, device_id_type=MESH)

    def cols(c, width):
        return pl.ds(pl.multiple_of(c * width, width), width)

    def source(kind, c):
        if kind == PACK:
            return pack
        if kind in (QKV0, QKV1):
            return wqkv.at[int(kind == QKV1), :, cols(c, QC)]
        return wup.at[int(kind == UP1), :, cols(c, FC)]

    def landing(kind, row):
        if kind == PACK:
            return packg.at[:, cols(row, ROWS)]
        if kind in (QKV0, QKV1):
            return wq.at[int(kind == QKV1), cols(row, ROWS), :]
        return wu.at[int(kind == UP1), cols(row, ROWS), :]

    def ici(kind, s):
        return remote(source(kind, chip_at(s)), landing(kind, me), ici_s.at[kind, s], ici_r.at[kind, s], peer(s))

    def ici_in(kind, s):
        return remote(source(kind, chip), landing(kind, peer(s)), ici_s.at[kind, s], ici_r.at[kind, s], peer(s))

    def d2d(kind, s):
        src = source(kind, chip) if s == 0 else landing(kind, peer(s))
        row = me if s == 0 else peer(s)
        return remote(src, landing(kind, row), d2d_s.at[kind, s], d2d_r.at[kind, s], partner)

    def d2d_in(kind, s):
        row = chip_at(s) * 2 + (1 - core)
        return remote(landing(kind, row), landing(kind, row), d2d_s.at[kind, s], d2d_r.at[kind, s], partner)

    def local(kind):
        return pltpu.make_async_copy(source(kind, chip), landing(kind, me), loc.at[kind])

    def own_refs(layer, which, core_index):
        if which == 0:
            return wout.at[layer], wo.at[layer, cols(core_index, ROWS), :]
        return wdown.at[layer], wd.at[layer, cols(core_index, DR), :]

    def own_remote(layer, which, core_index):
        src, dst = own_refs(layer, which, core_index)
        return remote(src, dst, own_s.at[layer, which], own_r.at[layer, which], partner)

    def own_local(layer, which):
        src, dst = own_refs(layer, which, core)
        return pltpu.make_async_copy(src, dst, own_l.at[layer, which])

    def send_block(kind, peers=(3, 1, 2)):
        for s in peers:
            ici(kind, s).start()

    def own_block(kind):
        local(kind).start()
        d2d(kind, 0).start()

    def own_rows(layer):
        for which in range(2):
            own_local(layer, which).start()
            own_remote(layer, which, core).start()

    def relay_block(kind):
        for s in (3, 1, 2):
            ici_in(kind, s).wait_recv()
            d2d(kind, s).start()

    def block_ready(kind):
        local(kind).wait()
        for s in range(4):
            d2d_in(kind, s).wait_recv()

    def own_ready(layer):
        for which in range(2):
            own_local(layer, which).wait()
            own_remote(layer, which, 1 - core).wait_recv()

    def h_half(j, half):
        return hg.at[j, :, cols(half, HALF)]

    def h_copy(layer, s, half):
        src = h_in.at[:, cols(half, HALF)] if layer == 0 else h_half(chip, half)
        return remote(src, h_half(chip, half), h_s.at[layer, s, half], h_r.at[layer, s, half], peer(s))

    def h_copy_in(layer, s, half):
        dst = h_half(chip_at(s), half)
        return remote(dst, dst, h_s.at[layer, s, half], h_r.at[layer, s, half], peer(s))

    def h_forward(layer, half):
        dst = h_half(chip_at(1 + half), half)
        return remote(dst, dst, hf_s.at[layer, half], hf_r.at[layer, half], peer(2 - half))

    def h_forward_in(layer, half):
        dst = h_half(chip_at(3), half)
        return remote(dst, dst, hf_s.at[layer, half], hf_r.at[layer, half], peer(2 - half))

    def h_send(layer):
        for s, half in ((1, 0), (2, 1), (1, 1), (2, 0)):
            h_copy(layer, s, half).start()

    def h_relay(layer):
        for half in range(2):
            h_copy_in(layer, 1 + half, half).wait_recv()
            h_forward(layer, half).start()

    def h_ready(layer):
        for half in range(2):
            h_copy_in(layer, 2 - half, half).wait_recv()
        for half in range(2):
            h_forward_in(layer, half).wait_recv()

    def h_sent(layer):
        for half in range(2):
            for s in (1, 2):
                h_copy(layer, s, half).wait_send()
            h_forward(layer, half).wait_send()

    def rs_copy(layer, n):
        s, half, to, dst = (
            (3, 0, 1, rsd.at[0]), (3, 1, 2, rsd.at[1]),
            (1, 0, 1, rsb.at[0]), (2, 1, 2, rsb.at[1]),
            (2, 0, 2, rsb.at[2]), (1, 1, 1, rsb.at[3]))[n]
        return remote(part.at[chip_at(s), half], dst, rs_s.at[layer, n], rs_r.at[layer, n], peer(to))

    def rs_pass_on(layer):
        for half in range(2):
            s = 2 - half
            rs_copy(layer, half).wait_recv()

            def step(i, carry):
                rows = pl.ds(pl.multiple_of(i * CH, CH), CH)
                part[chip_at(s), half, rows, :] = part[chip_at(s), half, rows, :] + rsd[half, rows, :]
                return carry

            lax.fori_loop(0, T // CH, step, 0)
            rs_copy(layer, 4 + half).start()

    def kv_copy(layer, which, s):
        src = (kr, vr)[which].at[chip_at(s)]
        dst = (kc, vc)[which].at[layer, chip]
        return remote(src, dst, kv_s.at[layer, which, s], kv_r.at[layer, which, s], peer(s))

    def kv_copy_in(layer, which, s):
        dst = (kc, vc)[which].at[layer, chip_at(s)]
        return remote(dst, dst, kv_s.at[layer, which, s], kv_r.at[layer, which, s], peer(s))

    def kv_local(layer, which):
        return pltpu.make_async_copy((kr, vr)[which].at[chip], (kc, vc)[which].at[layer, chip], kv_l.at[layer, which])

    def kv_send(layer):
        for which in range(2):
            kv_local(layer, which).start()
            for s in (3, 1, 2):
                kv_copy(layer, which, s).start()

    def kv_sent(layer):
        for which in range(2):
            kv_local(layer, which).wait()
            for s in (3, 1, 2):
                kv_copy(layer, which, s).wait_send()

    def norm(j, gain_row):
        gain = packg[gain_row:gain_row + 1, :]
        bias = packg[gain_row + 2:gain_row + 3, :]

        def step(i, carry):
            rows = pl.ds(pl.multiple_of(i * CH, CH), CH)
            x = hg[j, rows, :].astype(F32)
            mean = jnp.sum(x, axis=-1, keepdims=True) * (1.0 / D)
            x = x - mean
            var = jnp.sum(x * x, axis=-1, keepdims=True) * (1.0 / D)
            nb[rows, :] = (x * lax.rsqrt(var + LN_EPS) * gain + bias).astype(BF16)
            return carry

        lax.fori_loop(0, T // CH, step, 0)

    def rope(u):
        u = u.astype(F32)
        lo, hi = u[:, :HD // 2], u[:, HD // 2:]
        cos, sin = cos_ref[...], sin_ref[...]
        return jnp.concatenate([lo * cos - hi * sin, hi * cos + lo * sin], axis=-1).astype(BF16)

    def attention(layer, j):
        norm(j, layer)

        def project(i, carry):
            n = cols(i, TN)
            qkv[:, n] = jnp.dot(nb[...], wq[layer, :, n], preferred_element_type=F32).astype(BF16)
            return carry

        lax.fori_loop(0, QC // TN, project, 0)
        key = rope(qkv[:, 2 * HD:3 * HD])
        kr[j] = key
        vr[j] = qkv[:, 3 * HD:4 * HD]
        length = packg[8:9, pl.ds(pl.multiple_of((j * 2 + core) * ROWS, ROWS), 128)][:, 0:1]
        query_pos = lax.broadcasted_iota(jnp.int32, (T, T), 0)
        key_pos = lax.broadcasted_iota(jnp.int32, (T, T), 1)
        allowed = (key_pos <= query_pos) & (key_pos.astype(F32) < length)
        for head in range(2):
            query = rope(qkv[:, head * HD:(head + 1) * HD])
            scores = lax.dot_general(query, key, (((1,), (1,)), ((), ())), preferred_element_type=F32) * (HD ** -0.5)
            scores = jnp.where(allowed, scores, -1e30)
            expo = jnp.exp(scores - jnp.max(scores, axis=-1, keepdims=True))
            prob = (expo / jnp.sum(expo, axis=-1, keepdims=True)).astype(BF16)
            ctx[j, :, head * HD:(head + 1) * HD] = jnp.dot(prob, vr[j], preferred_element_type=F32).astype(BF16)

    def mlp(layer, j):
        norm(j, 4 + layer)

        def up(i, carry):
            n = cols(i, TN)
            u = jnp.dot(nb[...], wu[layer, :, n], preferred_element_type=F32)
            mid[:, n] = (0.5 * u * (1.0 + lax.erf(u * np.float32(np.sqrt(0.5))))).astype(BF16)
            return carry

        lax.fori_loop(0, FC // TN, up, 0)

        def down(i, carry):
            n = cols(i, TN)
            acc = jnp.dot(mid[...], wd[layer, :, n], preferred_element_type=F32)
            acc = acc + jnp.dot(ctx[j], wo[layer, :, n], preferred_element_type=F32)
            part[j, i // (HALF // TN), :, cols(i % (HALF // TN), TN)] = acc
            return carry

        lax.fori_loop(0, D // TN, down, 0)

    def residual(layer):
        for n in range(2, 6):
            rs_copy(layer, n).wait_recv()

        def step(i, carry):
            rows = pl.ds(pl.multiple_of(i * CH, CH), CH)
            for half in range(2):
                n = cols(half, HALF)
                total = hg[chip, rows, n].astype(F32) + part[chip, half, rows, :]
                hg[chip, rows, n] = (total + rsb[half, rows, :] + rsb[2 + half, rows, :]).astype(BF16)
            return carry

        lax.fori_loop(0, T // CH, step, 0)

    def attend_all(layer, first):
        def step(s, carry):
            attention(layer, chip_at(s))
            return carry

        lax.fori_loop(first, 4, step, 0)

    def mlp_all(layer):
        def step(i, carry):
            s = 3 - i
            mlp(layer, chip_at(s))
            for n, at in ((0, 3), (1, 3), (2, 1), (3, 2)):
                @pl.when(s == at)
                def _():
                    rs_copy(layer, n).start()
            return carry

        lax.fori_loop(0, 4, step, 0)

    barrier = pltpu.get_barrier_semaphore()
    for s in (1, 2, 3):
        pl.semaphore_signal(barrier, inc=1, device_id={"fsdp": peer(s)}, device_id_type=MESH)
    pl.semaphore_signal(barrier, inc=1, device_id={"fsdp": partner}, device_id_type=MESH)
    pl.semaphore_wait(barrier, 4)

    send_block(PACK)
    own_block(PACK)
    h_send(0)
    h_local = pltpu.make_async_copy(h_in, hg.at[chip], h_l.at[0])
    h_local.start()
    send_block(QKV0)
    own_block(QKV0)
    own_block(UP0)
    own_rows(0)
    relay_block(PACK)
    block_ready(PACK)
    h_relay(0)
    send_block(UP0)
    h_local.wait()
    h_ready(0)
    relay_block(QKV0)
    block_ready(QKV0)
    attend_all(0, 0)
    kv_send(0)
    send_block(QKV1)
    own_block(QKV1)
    own_block(UP1)
    own_rows(1)
    relay_block(UP0)
    block_ready(UP0)
    own_ready(0)
    h_sent(0)
    mlp_all(0)
    rs_pass_on(0)
    send_block(UP1, (3,))
    relay_block(QKV1)
    block_ready(QKV1)
    residual(0)
    h_send(1)
    kv_sent(0)
    attention(1, chip)
    h_relay(1)
    send_block(UP1, (1, 2))
    h_ready(1)
    attend_all(1, 1)
    kv_send(1)
    relay_block(UP1)
    block_ready(UP1)
    own_ready(1)
    for n in range(6):
        rs_copy(0, n).wait_send()
    mlp_all(1)
    rs_pass_on(1)
    h_sent(1)
    residual(1)
    final = pltpu.make_async_copy(hg.at[chip], h_out, out_l.at[0])
    final.start()

    for kind in range(5):
        for s in (3, 1, 2):
            ici(kind, s).wait_send()
        for s in range(4):
            d2d(kind, s).wait_send()
    for layer in range(2):
        for which in range(2):
            own_remote(layer, which, core).wait_send()
    for n in range(6):
        rs_copy(1, n).wait_send()
    kv_sent(1)
    for layer in range(2):
        for which in range(2):
            for s in (3, 1, 2):
                kv_copy_in(layer, which, s).wait_recv()
    final.wait()


def rope_tables():
    half = HD // 2
    inv_freq = np.float32(ROPE_BASE) ** (np.float32(-2.0) * np.arange(half, dtype=np.float32) / np.float32(HD))
    angles = np.arange(T, dtype=np.float32)[:, None] * inv_freq.astype(np.float32)[None, :]
    return np.cos(angles).astype(np.float32), np.sin(angles).astype(np.float32)


def solution(mesh):
    batch_spec = P(("dp", "fsdp"))
    weight_spec = P(None, "fsdp")
    cache_spec = P(None, ("dp", "fsdp"))
    vmem = pl.BlockSpec(memory_space=pltpu.VMEM)
    hbm = pl.BlockSpec(memory_space=pl.ANY)
    dma = pltpu.SemaphoreType.DMA

    def per_device(hidden_in, lengths, ln_attn_g, ln_attn_b, ln_mlp_g, ln_mlp_b, w_qkv, w_out, w_up, w_down):
        length_rows = jnp.broadcast_to(lengths.astype(F32)[:, None], (8, ROWS))
        pack = jnp.concatenate([ln_attn_g, ln_attn_b, ln_mlp_g, ln_mlp_b, length_rows], axis=0)
        cos, sin = rope_tables()
        call = pl.pallas_call(
            kernel,
            out_shape=(
                jax.ShapeDtypeStruct((T, D), BF16),
                jax.ShapeDtypeStruct((2, 4, T, HD), BF16),
                jax.ShapeDtypeStruct((2, 4, T, HD), BF16),
            ),
            in_specs=[vmem, hbm, hbm, hbm, hbm, hbm, vmem, vmem],
            out_specs=(hbm, hbm, hbm),
            scratch_shapes=[
                pltpu.VMEM((16, D), F32),
                pltpu.VMEM((2, D, QC), BF16),
                pltpu.VMEM((2, D, FC), BF16),
                pltpu.VMEM((2, 2 * ROWS, D), BF16),
                pltpu.VMEM((2, 2 * DR, D), BF16),
                pltpu.VMEM((4, T, D), BF16),
                pltpu.VMEM((4, 2, T, HALF), F32),
                pltpu.VMEM((2, T, HALF), F32),
                pltpu.VMEM((4, T, HALF), F32),
                pltpu.VMEM((T, D), BF16),
                pltpu.VMEM((T, QC), BF16),
                pltpu.VMEM((4, T, 2 * HD), BF16),
                pltpu.VMEM((4, T, HD), BF16),
                pltpu.VMEM((4, T, HD), BF16),
                pltpu.VMEM((T, FC), BF16),
                dma((5, 4)), dma((5, 4)), dma((5, 4)), dma((5, 4)), dma((5,)),
                dma((2, 2)), dma((2, 2)), dma((2, 2)),
                dma((2, 3, 2)), dma((2, 3, 2)), dma((2, 2)), dma((2, 2)), dma((1,)),
                dma((2, 6)), dma((2, 6)),
                dma((2, 2, 4)), dma((2, 2, 4)), dma((2, 2)), dma((1,)),
            ],
            compiler_params=pltpu.CompilerParams(
                collective_id=0, has_side_effects=True, vmem_limit_bytes=67043328),
            name="decoder_layers",
        )
        h_out, kc, vc = call(pack, hidden_in[0], w_qkv.reshape(2, ROWS, 4 * QC), w_out, w_up, w_down, cos, sin)
        return h_out[None], kc[:, None], vc[:, None]

    return jax.shard_map(per_device, mesh=mesh, in_specs=(batch_spec, batch_spec) + (weight_spec,) * 8, out_specs=(batch_spec, cache_spec, cache_spec), check_vma=False)
```

```python
import jax
import jax.numpy as jnp
import numpy as np
from jax import lax
from jax.experimental import pallas as pl
from jax.experimental.pallas import tpu as pltpu
from jax.sharding import PartitionSpec as P

MESH = pl.DeviceIdType.MESH
LN_EPS = 1e-5
ROPE_BASE = 10000.0
T = 192
D = 2048
HD = 256
ROWS = 256
QC = 1024
FC = 2048
DR = 1024
HALF = D // 2
RAW = 32
CH = 16
TN = 256
F32 = jnp.float32
BF16 = jnp.bfloat16
PACK, QKV0, UP0, QKV1, UP1 = range(5)


def kernel(len_ref, ga_ref, ba_ref, gm_ref, bm_ref, h_in, wqkv, wout, wup, wdown, cos_ref, sin_ref,
           h_out, kc, vc,
           pack, raw, packg, wq, wu, wo, wd, hg, part, rsd, rsb, nb, qkv, ctx, kr, vr, mid,
           ici_s, ici_r, d2d_s, d2d_r, loc, own_s, own_r, own_l,
           raw_l, h_s, h_r, hf_s, hf_r, h_l, rs_s, rs_r, kv_s, kv_r, kv_l, out_l):
    me = lax.axis_index("fsdp")
    core = me % 2
    chip = me // 2
    partner = chip * 2 + (1 - core)

    def chip_at(s):
        return ((chip // 2 + s // 2) % 2) * 2 + (chip % 2 + s % 2) % 2

    def peer(s):
        return chip_at(s) * 2 + core

    def remote(src, dst, send, recv, device):
        return pltpu.make_async_remote_copy(
            src_ref=src, dst_ref=dst, send_sem=send, recv_sem=recv,
            device_id={"fsdp": device}, device_id_type=MESH)

    def cols(c, width):
        return pl.ds(pl.multiple_of(c * width, width), width)

    def source(kind, c):
        if kind == PACK:
            return pack
        if kind in (QKV0, QKV1):
            return wd.at[1, pl.ds(pl.multiple_of(core * DR + int(kind == QKV1) * 2 * ROWS + (c // 2) * ROWS, ROWS), ROWS), cols(c % 2, QC)]
        return wup.at[int(kind == UP1), :, cols(c, FC)]

    def landing(kind, row):
        if kind == PACK:
            return packg.at[:, cols(row, ROWS)]
        if kind in (QKV0, QKV1):
            return wq.at[int(kind == QKV1), cols(row, ROWS), :]
        return wu.at[int(kind == UP1), cols(row, ROWS), :]

    def ici(kind, s):
        return remote(source(kind, chip_at(s)), landing(kind, me), ici_s.at[kind, s], ici_r.at[kind, s], peer(s))

    def ici_in(kind, s):
        return remote(source(kind, chip), landing(kind, peer(s)), ici_s.at[kind, s], ici_r.at[kind, s], peer(s))

    def d2d(kind, s):
        src = source(kind, chip) if s == 0 else landing(kind, peer(s))
        row = me if s == 0 else peer(s)
        return remote(src, landing(kind, row), d2d_s.at[kind, s], d2d_r.at[kind, s], partner)

    def d2d_in(kind, s):
        row = chip_at(s) * 2 + (1 - core)
        return remote(landing(kind, row), landing(kind, row), d2d_s.at[kind, s], d2d_r.at[kind, s], partner)

    def local(kind):
        return pltpu.make_async_copy(source(kind, chip), landing(kind, me), loc.at[kind])

    def own_refs(layer, which, core_index):
        if which == 0:
            return wout.at[layer], wo.at[layer, cols(core_index, ROWS), :]
        return wdown.at[layer], wd.at[layer, cols(core_index, DR), :]

    def own_remote(layer, which, core_index):
        src, dst = own_refs(layer, which, core_index)
        return remote(src, dst, own_s.at[layer, which], own_r.at[layer, which], partner)

    def own_local(layer, which):
        src, dst = own_refs(layer, which, core)
        return pltpu.make_async_copy(src, dst, own_l.at[layer, which])

    def raw_copy(layer, n, slot):
        return pltpu.make_async_copy(wqkv.at[layer, pl.ds(n * RAW, RAW)], raw.at[slot], raw_l.at[slot])

    def flatten_qkv(layer):
        raw_copy(layer, 0, 0).start()

        def step(n, carry):
            slot = n % 2

            @pl.when(n + 1 < ROWS // RAW)
            def _():
                raw_copy(layer, n + 1, 1 - slot).start()

            raw_copy(layer, n, slot).wait()
            for group in range(4):
                first = core * DR + layer * 2 * ROWS + (group // 2) * ROWS
                rows = pl.ds(pl.multiple_of(first + n * RAW, RAW), RAW)
                for part_of in range(4):
                    at = (group % 2) * QC + part_of * HD
                    wd[1, rows, at:at + HD] = raw[slot, :, group, part_of, :]
            return carry

        lax.fori_loop(0, ROWS // RAW, step, 0)

    def send_block(kind, peers=(3, 1, 2)):
        for s in peers:
            ici(kind, s).start()

    def own_block(kind):
        local(kind).start()
        d2d(kind, 0).start()

    def own_rows(layer):
        for which in range(2):
            own_local(layer, which).start()
            own_remote(layer, which, core).start()

    def relay_block(kind):
        for s in (3, 1, 2):
            ici_in(kind, s).wait_recv()
            d2d(kind, s).start()

    def block_ready(kind):
        local(kind).wait()
        for s in range(4):
            d2d_in(kind, s).wait_recv()

    def own_ready(layer):
        for which in range(2):
            own_local(layer, which).wait()
            own_remote(layer, which, 1 - core).wait_recv()

    def h_half(j, half):
        return hg.at[j, :, cols(half, HALF)]

    def h_copy(layer, s, half):
        src = h_in.at[:, cols(half, HALF)] if layer == 0 else h_half(chip, half)
        return remote(src, h_half(chip, half), h_s.at[layer, s, half], h_r.at[layer, s, half], peer(s))

    def h_copy_in(layer, s, half):
        dst = h_half(chip_at(s), half)
        return remote(dst, dst, h_s.at[layer, s, half], h_r.at[layer, s, half], peer(s))

    def h_forward(layer, half):
        dst = h_half(chip_at(1 + half), half)
        return remote(dst, dst, hf_s.at[layer, half], hf_r.at[layer, half], peer(2 - half))

    def h_forward_in(layer, half):
        dst = h_half(chip_at(3), half)
        return remote(dst, dst, hf_s.at[layer, half], hf_r.at[layer, half], peer(2 - half))

    def h_send(layer):
        for s, half in ((1, 0), (2, 1), (1, 1), (2, 0)):
            h_copy(layer, s, half).start()

    def h_relay(layer):
        for half in range(2):
            h_copy_in(layer, 1 + half, half).wait_recv()
            h_forward(layer, half).start()

    def h_ready(layer):
        for half in range(2):
            h_copy_in(layer, 2 - half, half).wait_recv()
        for half in range(2):
            h_forward_in(layer, half).wait_recv()

    def h_sent(layer):
        for half in range(2):
            for s in (1, 2):
                h_copy(layer, s, half).wait_send()
            h_forward(layer, half).wait_send()

    def rs_copy(layer, n):
        s, half, to, dst = (
            (3, 0, 1, rsd.at[0]), (3, 1, 2, rsd.at[1]),
            (1, 0, 1, rsb.at[0]), (2, 1, 2, rsb.at[1]),
            (2, 0, 2, rsb.at[2]), (1, 1, 1, rsb.at[3]))[n]
        return remote(part.at[chip_at(s), half], dst, rs_s.at[layer, n], rs_r.at[layer, n], peer(to))

    def rs_pass_on(layer):
        for half in range(2):
            s = 2 - half
            rs_copy(layer, half).wait_recv()

            def step(i, carry):
                rows = pl.ds(pl.multiple_of(i * CH, CH), CH)
                part[chip_at(s), half, rows, :] = part[chip_at(s), half, rows, :] + rsd[half, rows, :]
                return carry

            lax.fori_loop(0, T // CH, step, 0)
            rs_copy(layer, 4 + half).start()

    def kv_copy(layer, which, s):
        src = (kr, vr)[which].at[chip_at(s)]
        dst = (kc, vc)[which].at[layer, chip]
        return remote(src, dst, kv_s.at[layer, which, s], kv_r.at[layer, which, s], peer(s))

    def kv_copy_in(layer, which, s):
        dst = (kc, vc)[which].at[layer, chip_at(s)]
        return remote(dst, dst, kv_s.at[layer, which, s], kv_r.at[layer, which, s], peer(s))

    def kv_local(layer, which):
        return pltpu.make_async_copy((kr, vr)[which].at[chip], (kc, vc)[which].at[layer, chip], kv_l.at[layer, which])

    def kv_send(layer):
        for which in range(2):
            kv_local(layer, which).start()
            for s in (3, 1, 2):
                kv_copy(layer, which, s).start()

    def kv_sent(layer):
        for which in range(2):
            kv_local(layer, which).wait()
            for s in (3, 1, 2):
                kv_copy(layer, which, s).wait_send()

    def norm(j, gain_row):
        gain = packg[gain_row:gain_row + 1, :]
        bias = packg[gain_row + 2:gain_row + 3, :]

        def step(i, carry):
            rows = pl.ds(pl.multiple_of(i * CH, CH), CH)
            x = hg[j, rows, :].astype(F32)
            mean = jnp.sum(x, axis=-1, keepdims=True) * (1.0 / D)
            x = x - mean
            var = jnp.sum(x * x, axis=-1, keepdims=True) * (1.0 / D)
            nb[rows, :] = (x * lax.rsqrt(var + LN_EPS) * gain + bias).astype(BF16)
            return carry

        lax.fori_loop(0, T // CH, step, 0)

    def rope(u):
        u = u.astype(F32)
        lo, hi = u[:, :HD // 2], u[:, HD // 2:]
        cos, sin = cos_ref[...], sin_ref[...]
        return jnp.concatenate([lo * cos - hi * sin, hi * cos + lo * sin], axis=-1).astype(BF16)

    def attention(layer, j):
        norm(j, layer)

        def project(i, carry):
            n = cols(i, TN)
            qkv[:, n] = jnp.dot(nb[...], wq[layer, :, n], preferred_element_type=F32).astype(BF16)
            return carry

        lax.fori_loop(0, QC // TN, project, 0)
        key = rope(qkv[:, 2 * HD:3 * HD])
        kr[j] = key
        vr[j] = qkv[:, 3 * HD:4 * HD]
        length = packg[8:9, pl.ds(pl.multiple_of((j * 2 + core) * ROWS, ROWS), 128)][:, 0:1]
        query_pos = lax.broadcasted_iota(jnp.int32, (T, T), 0)
        key_pos = lax.broadcasted_iota(jnp.int32, (T, T), 1)
        allowed = (key_pos <= query_pos) & (key_pos.astype(F32) < length)
        for head in range(2):
            query = rope(qkv[:, head * HD:(head + 1) * HD])
            scores = lax.dot_general(query, key, (((1,), (1,)), ((), ())), preferred_element_type=F32) * (HD ** -0.5)
            scores = jnp.where(allowed, scores, -1e30)
            expo = jnp.exp(scores - jnp.max(scores, axis=-1, keepdims=True))
            prob = (expo / jnp.sum(expo, axis=-1, keepdims=True)).astype(BF16)
            ctx[j, :, head * HD:(head + 1) * HD] = jnp.dot(prob, vr[j], preferred_element_type=F32).astype(BF16)

    def mlp(layer, j):
        norm(j, 4 + layer)

        def up(i, carry):
            n = cols(i, TN)
            u = jnp.dot(nb[...], wu[layer, :, n], preferred_element_type=F32)
            mid[:, n] = (0.5 * u * (1.0 + lax.erf(u * np.float32(np.sqrt(0.5))))).astype(BF16)
            return carry

        lax.fori_loop(0, FC // TN, up, 0)

        def down(i, carry):
            n = cols(i, TN)
            acc = jnp.dot(mid[...], wd[layer, :, n], preferred_element_type=F32)
            acc = acc + jnp.dot(ctx[j], wo[layer, :, n], preferred_element_type=F32)
            part[j, i // (HALF // TN), :, cols(i % (HALF // TN), TN)] = acc
            return carry

        lax.fori_loop(0, D // TN, down, 0)

    def residual(layer):
        for n in range(2, 6):
            rs_copy(layer, n).wait_recv()

        def step(i, carry):
            rows = pl.ds(pl.multiple_of(i * CH, CH), CH)
            for half in range(2):
                n = cols(half, HALF)
                total = hg[chip, rows, n].astype(F32) + part[chip, half, rows, :]
                hg[chip, rows, n] = (total + rsb[half, rows, :] + rsb[2 + half, rows, :]).astype(BF16)
            return carry

        lax.fori_loop(0, T // CH, step, 0)

    def qkv_sent():
        for kind in (QKV0, QKV1):
            for s in (3, 1, 2):
                ici(kind, s).wait_send()
            d2d(kind, 0).wait_send()

    def attend_all(layer, first):
        def step(s, carry):
            attention(layer, chip_at(s))
            return carry

        lax.fori_loop(first, 4, step, 0)

    def mlp_all(layer):
        def step(i, carry):
            s = 3 - i
            mlp(layer, chip_at(s))
            for n, at in ((0, 3), (1, 3), (2, 1), (3, 2)):
                @pl.when(s == at)
                def _():
                    rs_copy(layer, n).start()
            return carry

        lax.fori_loop(0, 4, step, 0)

    barrier = pltpu.get_barrier_semaphore()
    for s in (1, 2, 3):
        pl.semaphore_signal(barrier, inc=1, device_id={"fsdp": peer(s)}, device_id_type=MESH)
    pl.semaphore_signal(barrier, inc=1, device_id={"fsdp": partner}, device_id_type=MESH)
    pl.semaphore_wait(barrier, 4)

    h_send(0)
    h_local = pltpu.make_async_copy(h_in, hg.at[chip], h_l.at[0])
    h_local.start()
    for n, ref in enumerate((ga_ref, ba_ref, gm_ref, bm_ref)):
        pack[2 * n:2 * n + 2, :] = ref[...]
    pack[8:16, :] = jnp.full((8, ROWS), len_ref[0].astype(F32), F32)
    flatten_qkv(0)
    send_block(PACK)
    own_block(PACK)
    send_block(QKV0)
    own_block(QKV0)
    own_block(UP0)
    own_rows(0)
    flatten_qkv(1)
    relay_block(PACK)
    block_ready(PACK)
    h_relay(0)
    send_block(UP0)
    h_local.wait()
    h_ready(0)
    relay_block(QKV0)
    block_ready(QKV0)
    attend_all(0, 0)
    kv_send(0)
    send_block(QKV1)
    own_block(QKV1)
    own_block(UP1)
    relay_block(UP0)
    block_ready(UP0)
    own_ready(0)
    h_sent(0)
    mlp_all(0)
    rs_pass_on(0)
    send_block(UP1, (3,))
    relay_block(QKV1)
    block_ready(QKV1)
    residual(0)
    h_send(1)
    qkv_sent()
    own_rows(1)
    kv_sent(0)
    attention(1, chip)
    h_relay(1)
    send_block(UP1, (1, 2))
    h_ready(1)
    attend_all(1, 1)
    kv_send(1)
    relay_block(UP1)
    block_ready(UP1)
    own_ready(1)
    for n in range(6):
        rs_copy(0, n).wait_send()
    mlp_all(1)
    rs_pass_on(1)
    h_sent(1)
    residual(1)
    final = pltpu.make_async_copy(hg.at[chip], h_out, out_l.at[0])
    final.start()

    for kind in range(5):
        for s in range(4):
            if kind not in (QKV0, QKV1):
                if s > 0:
                    ici(kind, s).wait_send()
                d2d(kind, s).wait_send()
            elif s > 0:
                d2d(kind, s).wait_send()
    for layer in range(2):
        for which in range(2):
            own_remote(layer, which, core).wait_send()
    for n in range(6):
        rs_copy(1, n).wait_send()
    kv_sent(1)
    for layer in range(2):
        for which in range(2):
            for s in (3, 1, 2):
                kv_copy_in(layer, which, s).wait_recv()
    final.wait()


def copy_out(h_in, k_in, v_in, h_out, k_out, v_out, h_buf, k_buf, v_buf, in_sem, out_sem):
    refs = ((h_in, h_buf, h_out), (k_in, k_buf, k_out), (v_in, v_buf, v_out))
    reads = [pltpu.make_async_copy(src, buf, in_sem.at[n]) for n, (src, buf, _) in enumerate(refs)]
    writes = [pltpu.make_async_copy(buf, dst, out_sem.at[n]) for n, (_, buf, dst) in enumerate(refs)]
    for read in reads:
        read.start()
    for read, write in zip(reads, writes):
        read.wait()
        write.start()
    for write in writes:
        write.wait()


def rope_tables():
    half = HD // 2
    inv_freq = np.float32(ROPE_BASE) ** (np.float32(-2.0) * np.arange(half, dtype=np.float32) / np.float32(HD))
    angles = np.arange(T, dtype=np.float32)[:, None] * inv_freq.astype(np.float32)[None, :]
    return np.cos(angles).astype(np.float32), np.sin(angles).astype(np.float32)


def solution(mesh):
    batch_spec = P(("dp", "fsdp"))
    weight_spec = P(None, "fsdp")
    cache_spec = P(None, ("dp", "fsdp"))
    vmem = pl.BlockSpec(memory_space=pltpu.VMEM)
    hbm = pl.BlockSpec(memory_space=pl.ANY)
    dma = pltpu.SemaphoreType.DMA

    def per_device(hidden_in, lengths, ln_attn_g, ln_attn_b, ln_mlp_g, ln_mlp_b, w_qkv, w_out, w_up, w_down):
        cos, sin = rope_tables()
        call = pl.pallas_call(
            kernel,
            out_shape=(
                jax.ShapeDtypeStruct((T, D), BF16),
                jax.ShapeDtypeStruct((2, 4, T, HD), BF16),
                jax.ShapeDtypeStruct((2, 4, T, HD), BF16),
            ),
            in_specs=[pl.BlockSpec(memory_space=pltpu.SMEM)] + [vmem] * 4 + [hbm] * 5 + [vmem] * 2,
            out_specs=(hbm, hbm, hbm),
            scratch_shapes=[
                pltpu.VMEM((16, ROWS), F32),
                pltpu.VMEM((2, RAW, 4, 4, HD), BF16),
                pltpu.VMEM((16, D), F32),
                pltpu.VMEM((2, D, QC), BF16),
                pltpu.VMEM((2, D, FC), BF16),
                pltpu.VMEM((2, 2 * ROWS, D), BF16),
                pltpu.VMEM((2, 2 * DR, D), BF16),
                pltpu.VMEM((4, T, D), BF16),
                pltpu.VMEM((4, 2, T, HALF), F32),
                pltpu.VMEM((2, T, HALF), F32),
                pltpu.VMEM((4, T, HALF), F32),
                pltpu.VMEM((T, D), BF16),
                pltpu.VMEM((T, QC), BF16),
                pltpu.VMEM((4, T, 2 * HD), BF16),
                pltpu.VMEM((4, T, HD), BF16),
                pltpu.VMEM((4, T, HD), BF16),
                pltpu.VMEM((T, FC), BF16),
                dma((5, 4)), dma((5, 4)), dma((5, 4)), dma((5, 4)), dma((5,)),
                dma((2, 2)), dma((2, 2)), dma((2, 2)),
                dma((2,)), dma((2, 3, 2)), dma((2, 3, 2)), dma((2, 2)), dma((2, 2)), dma((1,)),
                dma((2, 6)), dma((2, 6)),
                dma((2, 2, 4)), dma((2, 2, 4)), dma((2, 2)), dma((1,)),
            ],
            compiler_params=pltpu.CompilerParams(
                collective_id=0, has_side_effects=True, vmem_limit_bytes=67043328),
            name="decoder_layers",
        )
        results = call(lengths, ln_attn_g, ln_attn_b, ln_mlp_g, ln_mlp_b, hidden_in[0], w_qkv, w_out, w_up, w_down, cos, sin)
        h_out, kc, vc = pl.pallas_call(
            copy_out,
            out_shape=tuple(jax.ShapeDtypeStruct(r.shape, r.dtype) for r in results),
            in_specs=[hbm] * 3,
            out_specs=(hbm,) * 3,
            scratch_shapes=[pltpu.VMEM(r.shape, r.dtype) for r in results] + [dma((3,)), dma((3,))],
            name="copy_out",
        )(*results)
        return h_out[None], kc[:, None], vc[:, None]

    return jax.shard_map(per_device, mesh=mesh, in_specs=(batch_spec, batch_spec) + (weight_spec,) * 8, out_specs=(batch_spec, cache_spec, cache_spec), check_vma=False)
```

```python
import jax
import jax.numpy as jnp
import numpy as np
from jax import lax
from jax.experimental import pallas as pl
from jax.experimental.pallas import tpu as pltpu
from jax.sharding import PartitionSpec as P

MESH = pl.DeviceIdType.MESH
LN_EPS = 1e-5
ROPE_BASE = 10000.0
T = 192
D = 2048
HD = 256
ROWS = 256
QC = 1024
FC = 2048
DR = 1024
HALF = D // 2
OUT = 3
UNROLL = 2
RAW = 32
CH = 16
TN = 256
F32 = jnp.float32
BF16 = jnp.bfloat16
PACK, QKV0, UP0, QKV1, UP1 = range(5)


def kernel(len_ref, ga_ref, ba_ref, gm_ref, bm_ref, h_in, wqkv, wout, wup, wdown, cos_ref, sin_ref,
           h_out, kc, vc,
           pack, raw, packg, wq, wu, wo, wd, hg, part, rsd, rsb, nb, qkv, ctx, kr, vr,
           ici_s, ici_r, d2d_s, d2d_r, loc, own_s, own_r, own_l,
           raw_l, h_s, h_r, hf_s, hf_r, h_l, rs_s, rs_r, kv_s, kv_r, kv_l, out_l):
    me = lax.axis_index("fsdp")
    core = me % 2
    chip = me // 2
    partner = chip * 2 + (1 - core)

    def chip_at(s):
        return ((chip // 2 + s // 2) % 2) * 2 + (chip % 2 + s % 2) % 2

    def peer(s):
        return chip_at(s) * 2 + core

    def remote(src, dst, send, recv, device):
        return pltpu.make_async_remote_copy(
            src_ref=src, dst_ref=dst, send_sem=send, recv_sem=recv,
            device_id={"fsdp": device}, device_id_type=MESH)

    def cols(c, width):
        return pl.ds(pl.multiple_of(c * width, width), width)

    def source(kind, c):
        if kind == PACK:
            return pack
        if kind in (QKV0, QKV1):
            return wd.at[1, pl.ds(pl.multiple_of(core * DR + int(kind == QKV1) * 2 * ROWS + (c // 2) * ROWS, ROWS), ROWS), cols(c % 2, QC)]
        return wup.at[int(kind == UP1), :, cols(c, FC)]

    def landing(kind, row):
        if kind == PACK:
            return packg.at[:, cols(row, ROWS)]
        if kind in (QKV0, QKV1):
            return wq.at[int(kind == QKV1), cols(row, ROWS), :]
        return wu.at[int(kind == UP1), cols(row, ROWS), :]

    def ici(kind, s):
        return remote(source(kind, chip_at(s)), landing(kind, me), ici_s.at[kind, s], ici_r.at[kind, s], peer(s))

    def ici_in(kind, s):
        return remote(source(kind, chip), landing(kind, peer(s)), ici_s.at[kind, s], ici_r.at[kind, s], peer(s))

    def d2d(kind, s):
        src = source(kind, chip) if s == 0 else landing(kind, peer(s))
        row = me if s == 0 else peer(s)
        return remote(src, landing(kind, row), d2d_s.at[kind, s], d2d_r.at[kind, s], partner)

    def d2d_in(kind, s):
        row = chip_at(s) * 2 + (1 - core)
        return remote(landing(kind, row), landing(kind, row), d2d_s.at[kind, s], d2d_r.at[kind, s], partner)

    def local(kind):
        return pltpu.make_async_copy(source(kind, chip), landing(kind, me), loc.at[kind])

    def own_refs(layer, which, core_index):
        if which == 0:
            return wout.at[layer], wo.at[layer, cols(core_index, ROWS), :]
        return wdown.at[layer], wd.at[layer, cols(core_index, DR), :]

    def own_remote(layer, which, core_index):
        src, dst = own_refs(layer, which, core_index)
        return remote(src, dst, own_s.at[layer, which], own_r.at[layer, which], partner)

    def own_local(layer, which):
        src, dst = own_refs(layer, which, core)
        return pltpu.make_async_copy(src, dst, own_l.at[layer, which])

    def raw_copy(layer, n, slot):
        return pltpu.make_async_copy(wqkv.at[layer, pl.ds(n * RAW, RAW)], raw.at[slot], raw_l.at[slot])

    def flatten_qkv(layer):
        raw_copy(layer, 0, 0).start()

        def step(n, carry):
            slot = n % 2

            @pl.when(n + 1 < ROWS // RAW)
            def _():
                raw_copy(layer, n + 1, 1 - slot).start()

            raw_copy(layer, n, slot).wait()
            for group in range(4):
                first = core * DR + layer * 2 * ROWS + (group // 2) * ROWS
                rows = pl.ds(pl.multiple_of(first + n * RAW, RAW), RAW)
                for part_of in range(4):
                    at = (group % 2) * QC + part_of * HD
                    wd[1, rows, at:at + HD] = raw[slot, :, group, part_of, :]
            return carry

        lax.fori_loop(0, ROWS // RAW, step, 0)

    def send_block(kind, peers=(3, 1, 2)):
        for s in peers:
            ici(kind, s).start()

    def own_block(kind):
        local(kind).start()
        d2d(kind, 0).start()

    def own_rows(layer):
        for which in range(2):
            own_local(layer, which).start()
            own_remote(layer, which, core).start()

    def relay_block(kind):
        for s in (3, 1, 2):
            ici_in(kind, s).wait_recv()
            d2d(kind, s).start()

    def block_ready(kind):
        local(kind).wait()
        for s in range(4):
            d2d_in(kind, s).wait_recv()

    def own_ready(layer):
        for which in range(2):
            own_local(layer, which).wait()
            own_remote(layer, which, 1 - core).wait_recv()

    def h_half(j, half):
        return hg.at[j, :, cols(half, HALF)]

    def h_copy(layer, s, half):
        src = h_in.at[:, cols(half, HALF)] if layer == 0 else h_half(chip, half)
        return remote(src, h_half(chip, half), h_s.at[layer, s, half], h_r.at[layer, s, half], peer(s))

    def h_copy_in(layer, s, half):
        dst = h_half(chip_at(s), half)
        return remote(dst, dst, h_s.at[layer, s, half], h_r.at[layer, s, half], peer(s))

    def h_forward(layer, half):
        dst = h_half(chip_at(1 + half), half)
        return remote(dst, dst, hf_s.at[layer, half], hf_r.at[layer, half], peer(2 - half))

    def h_forward_in(layer, half):
        dst = h_half(chip_at(3), half)
        return remote(dst, dst, hf_s.at[layer, half], hf_r.at[layer, half], peer(2 - half))

    def h_send(layer):
        for s, half in ((1, 0), (2, 1), (1, 1), (2, 0)):
            h_copy(layer, s, half).start()

    def h_relay(layer):
        for half in range(2):
            h_copy_in(layer, 1 + half, half).wait_recv()
            h_forward(layer, half).start()

    def h_forwarded(layer):
        for half in range(2):
            h_forward(layer, half).wait_send()

    def h_ready(layer):
        h_forwarded(layer)
        for half in range(2):
            h_copy_in(layer, 2 - half, half).wait_recv()
        for half in range(2):
            h_forward_in(layer, half).wait_recv()

    def h_sent(layer):
        for half in range(2):
            for s in (1, 2):
                h_copy(layer, s, half).wait_send()

    def rs_copy(layer, n):
        s, half, to, dst = (
            (3, 0, 1, rsd.at[0]), (3, 1, 2, rsd.at[1]),
            (1, 0, 1, rsb.at[0]), (2, 1, 2, rsb.at[1]),
            (2, 0, 2, rsb.at[2]), (1, 1, 1, rsb.at[3]))[n]
        return remote(part.at[chip_at(s), half], dst, rs_s.at[layer, n], rs_r.at[layer, n], peer(to))

    def rs_pass_on(layer):
        for half in range(2):
            s = 2 - half
            rs_copy(layer, half).wait_recv()

            def step(i, carry):
                rows = pl.ds(pl.multiple_of(i * CH, CH), CH)
                part[chip_at(s), half, rows, :] = part[chip_at(s), half, rows, :] + rsd[half, rows, :]
                return carry

            lax.fori_loop(0, T // CH, step, 0)
            rs_copy(layer, 4 + half).start()

    def kv_copy(layer, which, s):
        src = (kr, vr)[which].at[layer, chip_at(s)]
        dst = (kc, vc)[which].at[layer, chip]
        return remote(src, dst, kv_s.at[layer, which, s], kv_r.at[layer, which, s], peer(s))

    def kv_copy_in(layer, which, s):
        dst = (kc, vc)[which].at[layer, chip_at(s)]
        return remote(dst, dst, kv_s.at[layer, which, s], kv_r.at[layer, which, s], peer(s))

    def kv_local(layer, which):
        return pltpu.make_async_copy((kr, vr)[which].at[layer, chip], (kc, vc)[which].at[layer, chip], kv_l.at[layer, which])

    def kv_send(layer):
        for which in range(2):
            kv_local(layer, which).start()
            for s in (3, 1, 2):
                kv_copy(layer, which, s).start()

    def kv_sent(layer):
        for which in range(2):
            kv_local(layer, which).wait()
            for s in (3, 1, 2):
                kv_copy(layer, which, s).wait_send()

    def hm_slot(s):
        own = 1 - (s + 3) // 4
        return own * 4 + (1 - own) * chip_at(s)

    def norm(layer, s):
        gain_a, bias_a, gain_m, bias_m = (packg[2 * n + layer:2 * n + layer + 1, :] for n in range(4))

        def step(i, carry):
            rows = pl.ds(pl.multiple_of(i * CH, CH), CH)
            x = hg[chip_at(s), rows, :].astype(F32)
            mean = jnp.sum(x, axis=-1, keepdims=True) * (1.0 / D)
            x = x - mean
            var = jnp.sum(x * x, axis=-1, keepdims=True) * (1.0 / D)
            x = x * lax.rsqrt(var + LN_EPS)
            nb[rows, :] = (x * gain_a + bias_a).astype(BF16)
            hg[hm_slot(s), rows, :] = (x * gain_m + bias_m).astype(BF16)
            return carry

        lax.fori_loop(0, T // CH, step, 0, unroll=UNROLL)

    def rope(u):
        u = u.astype(F32)
        lo, hi = u[:, :HD // 2], u[:, HD // 2:]
        cos, sin = cos_ref[...], sin_ref[...]
        return jnp.concatenate([lo * cos - hi * sin, hi * cos + lo * sin], axis=-1).astype(BF16)

    def attention(layer, s):
        j = chip_at(s)
        norm(layer, s)

        def project(i, carry):
            n = cols(i, TN)
            qkv[:, n] = jnp.dot(nb[...], wq[layer, :, n], preferred_element_type=F32).astype(BF16)
            return carry

        lax.fori_loop(0, QC // TN, project, 0)
        key = rope(qkv[:, 2 * HD:3 * HD])
        kr[layer, j] = key
        vr[layer, j] = qkv[:, 3 * HD:4 * HD]
        length = packg[8:9, pl.ds(pl.multiple_of((j * 2 + core) * ROWS, ROWS), 128)][:, 0:1]
        query_pos = lax.broadcasted_iota(jnp.int32, (T, T), 0)
        key_pos = lax.broadcasted_iota(jnp.int32, (T, T), 1)
        allowed = (key_pos <= query_pos) & (key_pos.astype(F32) < length)
        for head in range(2):
            query = rope(qkv[:, head * HD:(head + 1) * HD])
            scores = lax.dot_general(query, key, (((1,), (1,)), ((), ())), preferred_element_type=F32) * (HD ** -0.5)
            scores = jnp.where(allowed, scores, -1e30)
            expo = jnp.exp(scores - jnp.max(scores, axis=-1, keepdims=True))
            prob = (expo / jnp.sum(expo, axis=-1, keepdims=True)).astype(BF16)
            ctx[j, :, head * HD:(head + 1) * HD] = jnp.dot(prob, vr[layer, j], preferred_element_type=F32).astype(BF16)

    def mlp(layer, s):
        j = chip_at(s)
        hm = hg.at[hm_slot(s)]

        def up(i, carry):
            n = cols(i, TN)
            u = jnp.dot(hm[...], wu[layer, :, n], preferred_element_type=F32)
            nb[:, n] = (0.5 * u * (1.0 + lax.erf(u * np.float32(np.sqrt(0.5))))).astype(BF16)
            return carry

        lax.fori_loop(0, FC // TN, up, 0)

        def down(i, carry):
            n = cols(i, TN)
            acc = jnp.dot(nb[...], wd[layer, :, n], preferred_element_type=F32)
            acc = acc + jnp.dot(ctx[j], wo[layer, :, n], preferred_element_type=F32)
            part[j, i // (HALF // TN), :, cols(i % (HALF // TN), TN)] = acc
            return carry

        lax.fori_loop(0, D // TN, down, 0)

    def residual(layer):
        for half in range(2):
            rs_copy(layer, 2 + half).wait_recv()

        def direct(i, carry):
            rows = pl.ds(pl.multiple_of(i * CH, CH), CH)
            for half in range(2):
                total = hg[chip, rows, cols(half, HALF)].astype(F32) + part[chip, half, rows, :]
                part[chip, half, rows, :] = total + rsb[half, rows, :]
            return carry

        lax.fori_loop(0, T // CH, direct, 0)
        for half in range(2):
            rs_copy(layer, 4 + half).wait_recv()

        def step(i, carry):
            rows = pl.ds(pl.multiple_of(i * CH, CH), CH)
            for half in range(2):
                hg[chip, rows, cols(half, HALF)] = (part[chip, half, rows, :] + rsb[2 + half, rows, :]).astype(BF16)
            return carry

        for n in range(OUT):
            lax.fori_loop(n * (T // CH // OUT), (n + 1) * (T // CH // OUT), step, 0)
            if layer == 1:
                out_copy(n).start()

    def out_copy(n):
        rows = pl.ds(n * (T // OUT), T // OUT)
        return pltpu.make_async_copy(hg.at[chip, rows, :], h_out.at[rows, :], out_l.at[n])

    def qkv_sent():
        for kind in (QKV0, QKV1):
            for s in (3, 1, 2):
                ici(kind, s).wait_send()
            d2d(kind, 0).wait_send()

    def attend_all(layer, first):
        def step(s, carry):
            attention(layer, s)
            return carry

        lax.fori_loop(first, 4, step, 0)

    def mlp_all(layer):
        def step(i, carry):
            s = 3 - i
            mlp(layer, s)
            for n, at in ((0, 3), (1, 3), (2, 1), (3, 2)):
                @pl.when(s == at)
                def _():
                    rs_copy(layer, n).start()
            return carry

        lax.fori_loop(0, 4, step, 0)

    barrier = pltpu.get_barrier_semaphore()
    for s in (1, 2, 3):
        pl.semaphore_signal(barrier, inc=1, device_id={"fsdp": peer(s)}, device_id_type=MESH)
    pl.semaphore_signal(barrier, inc=1, device_id={"fsdp": partner}, device_id_type=MESH)
    pl.semaphore_wait(barrier, 4)

    h_send(0)
    h_local = pltpu.make_async_copy(h_in, hg.at[chip], h_l.at[0])
    h_local.start()
    for n, ref in enumerate((ga_ref, ba_ref, gm_ref, bm_ref)):
        pack[2 * n:2 * n + 2, :] = ref[...]
    pack[8:16, :] = jnp.full((8, ROWS), len_ref[0].astype(F32), F32)
    flatten_qkv(0)
    send_block(PACK)
    own_block(PACK)
    send_block(QKV0)
    own_block(QKV0)
    own_block(UP0)
    own_rows(0)
    flatten_qkv(1)
    relay_block(PACK)
    block_ready(PACK)
    h_relay(0)
    send_block(UP0)
    h_local.wait()
    h_ready(0)
    relay_block(QKV0)
    block_ready(QKV0)
    attend_all(0, 0)
    send_block(QKV1)
    own_block(QKV1)
    own_block(UP1)
    relay_block(UP0)
    block_ready(UP0)
    own_ready(0)
    h_sent(0)
    mlp_all(0)
    rs_pass_on(0)
    send_block(UP1, (3,))
    relay_block(QKV1)
    block_ready(QKV1)
    residual(0)
    h_send(1)
    qkv_sent()
    own_rows(1)
    attention(1, 0)
    h_relay(1)
    send_block(UP1, (1, 2))
    kv_send(0)
    h_ready(1)
    attend_all(1, 1)
    kv_send(1)
    relay_block(UP1)
    block_ready(UP1)
    own_ready(1)
    for n in range(6):
        rs_copy(0, n).wait_send()
    mlp_all(1)
    rs_pass_on(1)
    h_sent(1)
    residual(1)

    for kind in range(5):
        for s in range(4):
            if kind not in (QKV0, QKV1):
                if s > 0:
                    ici(kind, s).wait_send()
                d2d(kind, s).wait_send()
            elif s > 0:
                d2d(kind, s).wait_send()
    for layer in range(2):
        for which in range(2):
            own_remote(layer, which, core).wait_send()
    for n in range(6):
        rs_copy(1, n).wait_send()
    kv_sent(0)
    kv_sent(1)
    for layer in range(2):
        for which in range(2):
            for s in (3, 1, 2):
                kv_copy_in(layer, which, s).wait_recv()
    for n in range(OUT):
        out_copy(n).wait()


def copy_out(h_in, k_in, v_in, h_out, k_out, v_out, h_buf, k_buf, v_buf, in_sem, out_sem):
    refs = ((h_in, h_buf, h_out), (k_in, k_buf, k_out), (v_in, v_buf, v_out))
    reads = [pltpu.make_async_copy(src, buf, in_sem.at[n]) for n, (src, buf, _) in enumerate(refs)]
    writes = [pltpu.make_async_copy(buf, dst, out_sem.at[n]) for n, (_, buf, dst) in enumerate(refs)]
    for read in reads:
        read.start()
    for read, write in zip(reads, writes):
        read.wait()
        write.start()
    for write in writes:
        write.wait()


def rope_tables():
    half = HD // 2
    inv_freq = np.float32(ROPE_BASE) ** (np.float32(-2.0) * np.arange(half, dtype=np.float32) / np.float32(HD))
    angles = np.arange(T, dtype=np.float32)[:, None] * inv_freq.astype(np.float32)[None, :]
    return np.cos(angles).astype(np.float32), np.sin(angles).astype(np.float32)


def solution(mesh):
    batch_spec = P(("dp", "fsdp"))
    weight_spec = P(None, "fsdp")
    cache_spec = P(None, ("dp", "fsdp"))
    vmem = pl.BlockSpec(memory_space=pltpu.VMEM)
    hbm = pl.BlockSpec(memory_space=pl.ANY)
    dma = pltpu.SemaphoreType.DMA

    def per_device(hidden_in, lengths, ln_attn_g, ln_attn_b, ln_mlp_g, ln_mlp_b, w_qkv, w_out, w_up, w_down):
        cos, sin = rope_tables()
        call = pl.pallas_call(
            kernel,
            out_shape=(
                jax.ShapeDtypeStruct((T, D), BF16),
                jax.ShapeDtypeStruct((2, 4, T, HD), BF16),
                jax.ShapeDtypeStruct((2, 4, T, HD), BF16),
            ),
            in_specs=[pl.BlockSpec(memory_space=pltpu.SMEM)] + [vmem] * 4 + [hbm] * 5 + [vmem] * 2,
            out_specs=(hbm, hbm, hbm),
            scratch_shapes=[
                pltpu.VMEM((16, ROWS), F32),
                pltpu.VMEM((2, RAW, 4, 4, HD), BF16),
                pltpu.VMEM((16, D), F32),
                pltpu.VMEM((2, D, QC), BF16),
                pltpu.VMEM((2, D, FC), BF16),
                pltpu.VMEM((2, 2 * ROWS, D), BF16),
                pltpu.VMEM((2, 2 * DR, D), BF16),
                pltpu.VMEM((5, T, D), BF16),
                pltpu.VMEM((4, 2, T, HALF), F32),
                pltpu.VMEM((2, T, HALF), F32),
                pltpu.VMEM((4, T, HALF), F32),
                pltpu.VMEM((T, D), BF16),
                pltpu.VMEM((T, QC), BF16),
                pltpu.VMEM((4, T, 2 * HD), BF16),
                pltpu.VMEM((2, 4, T, HD), BF16),
                pltpu.VMEM((2, 4, T, HD), BF16),
                dma((5, 4)), dma((5, 4)), dma((5, 4)), dma((5, 4)), dma((5,)),
                dma((2, 2)), dma((2, 2)), dma((2, 2)),
                dma((2,)), dma((2, 3, 2)), dma((2, 3, 2)), dma((2, 2)), dma((2, 2)), dma((1,)),
                dma((2, 6)), dma((2, 6)),
                dma((2, 2, 4)), dma((2, 2, 4)), dma((2, 2)), dma((OUT,)),
            ],
            compiler_params=pltpu.CompilerParams(
                collective_id=0, has_side_effects=True, vmem_limit_bytes=67043328),
            name="decoder_layers",
        )
        results = call(lengths, ln_attn_g, ln_attn_b, ln_mlp_g, ln_mlp_b, hidden_in[0], w_qkv, w_out, w_up, w_down, cos, sin)
        h_out, kc, vc = pl.pallas_call(
            copy_out,
            out_shape=tuple(jax.ShapeDtypeStruct(r.shape, r.dtype) for r in results),
            in_specs=[hbm] * 3,
            out_specs=(hbm,) * 3,
            scratch_shapes=[pltpu.VMEM(r.shape, r.dtype) for r in results] + [dma((3,)), dma((3,))],
            name="copy_out",
        )(*results)
        return h_out[None], kc[:, None], vc[:, None]

    return jax.shard_map(per_device, mesh=mesh, in_specs=(batch_spec, batch_spec) + (weight_spec,) * 8, out_specs=(batch_spec, cache_spec, cache_spec), check_vma=False)
```

```python
import jax
import jax.numpy as jnp
import numpy as np
from jax import lax
from jax.experimental import pallas as pl
from jax.experimental.pallas import tpu as pltpu
from jax.sharding import PartitionSpec as P

MESH = pl.DeviceIdType.MESH
LN_EPS = 1e-5
ROPE_BASE = 10000.0
T = 192
D = 2048
HD = 256
ROWS = 256
QC = 1024
FC = 2048
DR = 1024
HALF = D // 2
UNROLL = 2
RAW = 32
CH = 16
TN = 256
F32 = jnp.float32
BF16 = jnp.bfloat16
PACK, QKV0, UP0, QKV1, UP1 = range(5)


def kernel(len_ref, ga_ref, ba_ref, gm_ref, bm_ref, h_in, wqkv, wout, wup, wdown, cos_hbm, sin_hbm,
           h_out, kc, vc,
           cos_ref, sin_ref, pack, raw, packg, wq, wu, wo, wd, hg, part, rsd, rsb, nb, qkv, ctx, kr, vr,
           ici_s, ici_r, d2d_s, d2d_r, loc, own_s, own_r, own_l,
           raw_l, h_s, h_r, hf_s, hf_r, h_l, rs_s, rs_r, kv_s, kv_r, kv_l, const_l, free):
    me = lax.axis_index("fsdp")
    core = me % 2
    chip = me // 2
    partner = chip * 2 + (1 - core)

    def chip_at(s):
        return ((chip // 2 + s // 2) % 2) * 2 + (chip % 2 + s % 2) % 2

    def peer(s):
        return chip_at(s) * 2 + core

    def remote(src, dst, send, recv, device):
        return pltpu.make_async_remote_copy(
            src_ref=src, dst_ref=dst, send_sem=send, recv_sem=recv,
            device_id={"fsdp": device}, device_id_type=MESH)

    def cols(c, width):
        return pl.ds(pl.multiple_of(c * width, width), width)

    def source(kind, c):
        if kind == PACK:
            return pack
        if kind in (QKV0, QKV1):
            return wd.at[1, pl.ds(pl.multiple_of(core * DR + int(kind == QKV1) * 2 * ROWS + (c // 2) * ROWS, ROWS), ROWS), cols(c % 2, QC)]
        return wup.at[int(kind == UP1), :, cols(c, FC)]

    def landing(kind, row):
        if kind == PACK:
            return packg.at[:, cols(row, ROWS)]
        if kind in (QKV0, QKV1):
            return wq.at[cols(row, ROWS), :]
        return wu.at[int(kind == UP1), cols(row, ROWS), :]

    def ici(kind, s):
        return remote(source(kind, chip_at(s)), landing(kind, me), ici_s.at[kind, s], ici_r.at[kind, s], peer(s))

    def ici_in(kind, s):
        return remote(source(kind, chip), landing(kind, peer(s)), ici_s.at[kind, s], ici_r.at[kind, s], peer(s))

    def d2d(kind, s):
        src = source(kind, chip) if s == 0 else landing(kind, peer(s))
        row = me if s == 0 else peer(s)
        return remote(src, landing(kind, row), d2d_s.at[kind, s], d2d_r.at[kind, s], partner)

    def d2d_in(kind, s):
        row = chip_at(s) * 2 + (1 - core)
        return remote(landing(kind, row), landing(kind, row), d2d_s.at[kind, s], d2d_r.at[kind, s], partner)

    def local(kind):
        return pltpu.make_async_copy(source(kind, chip), landing(kind, me), loc.at[kind])

    def own_refs(layer, which, core_index):
        if which == 0:
            return wout.at[layer], wo.at[layer, cols(core_index, ROWS), :]
        return wdown.at[layer], wd.at[layer, cols(core_index, DR), :]

    def own_remote(layer, which, core_index):
        src, dst = own_refs(layer, which, core_index)
        return remote(src, dst, own_s.at[layer, which], own_r.at[layer, which], partner)

    def own_local(layer, which):
        src, dst = own_refs(layer, which, core)
        return pltpu.make_async_copy(src, dst, own_l.at[layer, which])

    def raw_copy(layer, n, slot):
        return pltpu.make_async_copy(wqkv.at[layer, pl.ds(n * RAW, RAW)], raw.at[slot], raw_l.at[slot])

    def flatten_qkv(layer):
        raw_copy(layer, 0, 0).start()

        def step(n, carry):
            slot = n % 2

            @pl.when(n + 1 < ROWS // RAW)
            def _():
                raw_copy(layer, n + 1, 1 - slot).start()

            raw_copy(layer, n, slot).wait()
            for group in range(4):
                first = core * DR + layer * 2 * ROWS + (group // 2) * ROWS
                rows = pl.ds(pl.multiple_of(first + n * RAW, RAW), RAW)
                for part_of in range(4):
                    at = (group % 2) * QC + part_of * HD
                    wd[1, rows, at:at + HD] = raw[slot, :, group, part_of, :]
            return carry

        lax.fori_loop(0, ROWS // RAW, step, 0)

    def send_block(kind, peers=(3, 1, 2)):
        for s in peers:
            ici(kind, s).start()

    def own_block(kind):
        local(kind).start()
        d2d(kind, 0).start()

    def own_rows(layer):
        for which in range(2):
            own_local(layer, which).start()
            own_remote(layer, which, core).start()

    def relay_block(kind):
        for s in (3, 1, 2):
            ici_in(kind, s).wait_recv()
            d2d(kind, s).start()

    def block_ready(kind):
        local(kind).wait()
        for s in range(4):
            d2d_in(kind, s).wait_recv()

    def own_ready(layer):
        for which in range(2):
            own_local(layer, which).wait()
            own_remote(layer, which, 1 - core).wait_recv()

    def h_half(j, half):
        return hg.at[j, :, cols(half, HALF)]

    def h_copy(layer, s, half):
        src = h_in.at[:, cols(half, HALF)] if layer == 0 else h_half(chip, half)
        return remote(src, h_half(chip, half), h_s.at[layer, s, half], h_r.at[layer, s, half], peer(s))

    def h_copy_in(layer, s, half):
        dst = h_half(chip_at(s), half)
        return remote(dst, dst, h_s.at[layer, s, half], h_r.at[layer, s, half], peer(s))

    def h_forward(layer, half):
        dst = h_half(chip_at(1 + half), half)
        return remote(dst, dst, hf_s.at[layer, half], hf_r.at[layer, half], peer(2 - half))

    def h_forward_in(layer, half):
        dst = h_half(chip_at(3), half)
        return remote(dst, dst, hf_s.at[layer, half], hf_r.at[layer, half], peer(2 - half))

    def h_send(layer):
        for s, half in ((1, 0), (2, 1), (1, 1), (2, 0)):
            h_copy(layer, s, half).start()

    def h_relay(layer):
        for half in range(2):
            h_copy_in(layer, 1 + half, half).wait_recv()
            h_forward(layer, half).start()

    def h_forwarded(layer):
        for half in range(2):
            h_forward(layer, half).wait_send()

    def h_ready(layer):
        h_forwarded(layer)
        for half in range(2):
            h_copy_in(layer, 2 - half, half).wait_recv()
        for half in range(2):
            h_forward_in(layer, half).wait_recv()

    def h_sent(layer):
        for half in range(2):
            for s in (1, 2):
                h_copy(layer, s, half).wait_send()

    def rs_copy(layer, n):
        s, half, to, dst = (
            (3, 0, 1, rsd.at[0]), (3, 1, 2, rsd.at[1]),
            (1, 0, 1, rsb.at[0]), (2, 1, 2, rsb.at[1]),
            (2, 0, 2, rsb.at[2]), (1, 1, 1, rsb.at[3]))[n]
        return remote(part.at[chip_at(s), half], dst, rs_s.at[layer, n], rs_r.at[layer, n], peer(to))

    def rs_pass_on(layer):
        for half in range(2):
            s = 2 - half
            rs_copy(layer, half).wait_recv()

            def step(i, carry):
                rows = pl.ds(pl.multiple_of(i * CH, CH), CH)
                part[chip_at(s), half, rows, :] = part[chip_at(s), half, rows, :] + rsd[half, rows, :]
                return carry

            lax.fori_loop(0, T // CH, step, 0)
            rs_copy(layer, 4 + half).start()

    def kv_copy(layer, which, s):
        src = (kr, vr)[which].at[layer, chip_at(s)]
        dst = (kc, vc)[which].at[layer, chip]
        return remote(src, dst, kv_s.at[layer, which, s], kv_r.at[layer, which, s], peer(s))

    def kv_copy_in(layer, which, s):
        dst = (kc, vc)[which].at[layer, chip_at(s)]
        return remote(dst, dst, kv_s.at[layer, which, s], kv_r.at[layer, which, s], peer(s))

    def kv_local(layer, which):
        return pltpu.make_async_copy((kr, vr)[which].at[layer, chip], (kc, vc)[which].at[layer, chip], kv_l.at[layer, which])

    def kv_send(layer):
        for which in range(2):
            kv_local(layer, which).start()
            for s in (3, 1, 2):
                kv_copy(layer, which, s).start()

    def kv_sent(layer):
        for which in range(2):
            kv_local(layer, which).wait()
            for s in (3, 1, 2):
                kv_copy(layer, which, s).wait_send()

    def hm_slot(s):
        own = 1 - (s + 3) // 4
        return own * 4 + (1 - own) * chip_at(s)

    def norm(layer, s):
        gain_a, bias_a, gain_m, bias_m = (packg[2 * n + layer:2 * n + layer + 1, :] for n in range(4))

        def step(i, carry):
            rows = pl.ds(pl.multiple_of(i * CH, CH), CH)
            x = hg[chip_at(s), rows, :].astype(F32)
            mean = jnp.sum(x, axis=-1, keepdims=True) * (1.0 / D)
            x = x - mean
            var = jnp.sum(x * x, axis=-1, keepdims=True) * (1.0 / D)
            x = x * lax.rsqrt(var + LN_EPS)
            nb[rows, :] = (x * gain_a + bias_a).astype(BF16)
            hg[hm_slot(s), rows, :] = (x * gain_m + bias_m).astype(BF16)
            return carry

        lax.fori_loop(0, T // CH, step, 0, unroll=UNROLL)

    def rope(u):
        u = u.astype(F32)
        lo, hi = u[:, :HD // 2], u[:, HD // 2:]
        cos, sin = cos_ref[...], sin_ref[...]
        return jnp.concatenate([lo * cos - hi * sin, hi * cos + lo * sin], axis=-1).astype(BF16)

    def attention(layer, s):
        j = chip_at(s)
        norm(layer, s)

        def project(i, carry):
            n = cols(i, TN)
            qkv[:, n] = jnp.dot(nb[...], wq[:, n], preferred_element_type=F32).astype(BF16)
            return carry

        lax.fori_loop(0, QC // TN, project, 0)
        key = rope(qkv[:, 2 * HD:3 * HD])
        kr[layer, j] = key
        vr[layer, j] = qkv[:, 3 * HD:4 * HD]
        length = packg[8:9, pl.ds(pl.multiple_of((j * 2 + core) * ROWS, ROWS), 128)][:, 0:1]
        query_pos = lax.broadcasted_iota(jnp.int32, (T, T), 0)
        key_pos = lax.broadcasted_iota(jnp.int32, (T, T), 1)
        allowed = (key_pos <= query_pos) & (key_pos.astype(F32) < length)
        for head in range(2):
            query = rope(qkv[:, head * HD:(head + 1) * HD])
            scores = lax.dot_general(query, key, (((1,), (1,)), ((), ())), preferred_element_type=F32) * (HD ** -0.5)
            scores = jnp.where(allowed, scores, -1e30)
            expo = jnp.exp(scores - jnp.max(scores, axis=-1, keepdims=True))
            prob = (expo / jnp.sum(expo, axis=-1, keepdims=True)).astype(BF16)
            ctx[j, :, head * HD:(head + 1) * HD] = jnp.dot(prob, vr[layer, j], preferred_element_type=F32).astype(BF16)

    def mlp(layer, s):
        j = chip_at(s)
        hm = hg.at[hm_slot(s)]

        def up(i, carry):
            n = cols(i, TN)
            u = jnp.dot(hm[...], wu[layer, :, n], preferred_element_type=F32)
            nb[:, n] = (0.5 * u * (1.0 + lax.erf(u * np.float32(np.sqrt(0.5))))).astype(BF16)
            return carry

        lax.fori_loop(0, FC // TN, up, 0)

        def down(i, carry):
            n = cols(i, TN)
            acc = jnp.dot(nb[...], wd[layer, :, n], preferred_element_type=F32)
            acc = acc + jnp.dot(ctx[j], wo[layer, :, n], preferred_element_type=F32)
            part[j, i // (HALF // TN), :, cols(i % (HALF // TN), TN)] = acc
            return carry

        lax.fori_loop(0, D // TN, down, 0)

    def residual(layer):
        for half in range(2):
            rs_copy(layer, 2 + half).wait_recv()

        def direct(i, carry):
            rows = pl.ds(pl.multiple_of(i * CH, CH), CH)
            for half in range(2):
                total = hg[chip, rows, cols(half, HALF)].astype(F32) + part[chip, half, rows, :]
                part[chip, half, rows, :] = total + rsb[half, rows, :]
            return carry

        lax.fori_loop(0, T // CH, direct, 0)
        for half in range(2):
            rs_copy(layer, 4 + half).wait_recv()

        def step(i, carry):
            rows = pl.ds(pl.multiple_of(i * CH, CH), CH)
            for half in range(2):
                total = (part[chip, half, rows, :] + rsb[2 + half, rows, :]).astype(BF16)
                if layer == 0:
                    hg[chip, rows, cols(half, HALF)] = total
                else:
                    h_out[rows, half * HALF:(half + 1) * HALF] = total
            return carry

        lax.fori_loop(0, T // CH, step, 0)

    def qkv_sent():
        for kind in (QKV0, QKV1):
            for s in (3, 1, 2):
                ici(kind, s).wait_send()
        d2d(QKV1, 0).wait_send()

    def attend_all(layer, first):
        def step(s, carry):
            attention(layer, s)
            return carry

        lax.fori_loop(first, 4, step, 0)

    def mlp_all(layer):
        def step(i, carry):
            s = 3 - i
            mlp(layer, s)
            for n, at in ((0, 3), (1, 3), (2, 1), (3, 2)):
                @pl.when(s == at)
                def _():
                    rs_copy(layer, n).start()
            return carry

        lax.fori_loop(0, 4, step, 0)

    barrier = pltpu.get_barrier_semaphore()
    for s in (1, 2, 3):
        pl.semaphore_signal(barrier, inc=1, device_id={"fsdp": peer(s)}, device_id_type=MESH)
    pl.semaphore_signal(barrier, inc=1, device_id={"fsdp": partner}, device_id_type=MESH)
    pl.semaphore_wait(barrier, 4)

    h_send(0)
    h_local = pltpu.make_async_copy(h_in, hg.at[chip], h_l.at[0])
    h_local.start()
    tables = [pltpu.make_async_copy(src, dst, const_l.at[n])
              for n, (src, dst) in enumerate(((cos_hbm, cos_ref), (sin_hbm, sin_ref)))]
    for table in tables:
        table.start()
    for n, ref in enumerate((ga_ref, ba_ref, gm_ref, bm_ref)):
        pack[2 * n:2 * n + 2, :] = ref[...]
    pack[8:16, :] = jnp.full((8, ROWS), len_ref[0].astype(F32), F32)
    flatten_qkv(0)
    send_block(PACK)
    own_block(PACK)
    send_block(QKV0)
    own_block(QKV0)
    own_block(UP0)
    own_rows(0)
    flatten_qkv(1)
    relay_block(PACK)
    block_ready(PACK)
    h_relay(0)
    send_block(UP0)
    h_local.wait()
    for table in tables:
        table.wait()
    h_ready(0)
    relay_block(QKV0)
    block_ready(QKV0)
    attend_all(0, 0)
    for s in range(4):
        d2d(QKV0, s).wait_send()
    for device in (peer(1), peer(2), peer(3), partner):
        pl.semaphore_signal(free, inc=1, device_id={"fsdp": device}, device_id_type=MESH)
    pl.semaphore_wait(free, 4)
    send_block(QKV1)
    own_block(QKV1)
    own_block(UP1)
    relay_block(UP0)
    block_ready(UP0)
    own_ready(0)
    h_sent(0)
    mlp_all(0)
    rs_pass_on(0)
    send_block(UP1, (3,))
    relay_block(QKV1)
    block_ready(QKV1)
    residual(0)
    h_send(1)
    qkv_sent()
    own_rows(1)
    attention(1, 0)
    h_relay(1)
    send_block(UP1, (1, 2))
    kv_send(0)
    h_ready(1)
    attend_all(1, 1)
    kv_send(1)
    relay_block(UP1)
    block_ready(UP1)
    own_ready(1)
    for n in range(6):
        rs_copy(0, n).wait_send()
    mlp_all(1)
    rs_pass_on(1)
    h_sent(1)
    residual(1)

    for kind in range(5):
        for s in range(4):
            if kind not in (QKV0, QKV1):
                if s > 0:
                    ici(kind, s).wait_send()
                d2d(kind, s).wait_send()
            elif kind == QKV1 and s > 0:
                d2d(kind, s).wait_send()
    for layer in range(2):
        for which in range(2):
            own_remote(layer, which, core).wait_send()
    for n in range(6):
        rs_copy(1, n).wait_send()
    kv_sent(0)
    kv_sent(1)
    for layer in range(2):
        for which in range(2):
            for s in (3, 1, 2):
                kv_copy_in(layer, which, s).wait_recv()


def copy_out(h_in, k_in, v_in, h_out, k_out, v_out, sem):
    pairs = ((h_in, h_out), (k_in, k_out), (v_in, v_out))
    writes = [pltpu.make_async_copy(src, dst, sem.at[n]) for n, (src, dst) in enumerate(pairs)]
    for write in writes:
        write.start()
    for write in writes:
        write.wait()


def rope_tables():
    half = HD // 2
    inv_freq = np.float32(ROPE_BASE) ** (np.float32(-2.0) * np.arange(half, dtype=np.float32) / np.float32(HD))
    angles = np.arange(T, dtype=np.float32)[:, None] * inv_freq.astype(np.float32)[None, :]
    return np.cos(angles).astype(np.float32), np.sin(angles).astype(np.float32)


def solution(mesh):
    batch_spec = P(("dp", "fsdp"))
    weight_spec = P(None, "fsdp")
    cache_spec = P(None, ("dp", "fsdp"))
    vmem = pl.BlockSpec(memory_space=pltpu.VMEM)
    hbm = pl.BlockSpec(memory_space=pl.ANY)
    dma = pltpu.SemaphoreType.DMA

    def per_device(hidden_in, lengths, ln_attn_g, ln_attn_b, ln_mlp_g, ln_mlp_b, w_qkv, w_out, w_up, w_down):
        cos, sin = rope_tables()
        call = pl.pallas_call(
            kernel,
            out_shape=(
                pltpu.VMEM((T, D), BF16),
                pltpu.VMEM((2, 4, T, HD), BF16),
                pltpu.VMEM((2, 4, T, HD), BF16),
            ),
            in_specs=[pl.BlockSpec(memory_space=pltpu.SMEM)] + [vmem] * 4 + [hbm] * 7,
            out_specs=(vmem, vmem, vmem),
            scratch_shapes=[
                pltpu.VMEM((T, HD // 2), F32),
                pltpu.VMEM((T, HD // 2), F32),
                pltpu.VMEM((16, ROWS), F32),
                pltpu.VMEM((2, RAW, 4, 4, HD), BF16),
                pltpu.VMEM((16, D), F32),
                pltpu.VMEM((D, QC), BF16),
                pltpu.VMEM((2, D, FC), BF16),
                pltpu.VMEM((2, 2 * ROWS, D), BF16),
                pltpu.VMEM((2, 2 * DR, D), BF16),
                pltpu.VMEM((5, T, D), BF16),
                pltpu.VMEM((4, 2, T, HALF), F32),
                pltpu.VMEM((2, T, HALF), F32),
                pltpu.VMEM((4, T, HALF), F32),
                pltpu.VMEM((T, D), BF16),
                pltpu.VMEM((T, QC), BF16),
                pltpu.VMEM((4, T, 2 * HD), BF16),
                pltpu.VMEM((2, 4, T, HD), BF16),
                pltpu.VMEM((2, 4, T, HD), BF16),
                dma((5, 4)), dma((5, 4)), dma((5, 4)), dma((5, 4)), dma((5,)),
                dma((2, 2)), dma((2, 2)), dma((2, 2)),
                dma((2,)), dma((2, 3, 2)), dma((2, 3, 2)), dma((2, 2)), dma((2, 2)), dma((1,)),
                dma((2, 6)), dma((2, 6)),
                dma((2, 2, 4)), dma((2, 2, 4)), dma((2, 2)), dma((2,)),
                pltpu.SemaphoreType.REGULAR,
            ],
            compiler_params=pltpu.CompilerParams(
                collective_id=0, has_side_effects=True, vmem_limit_bytes=64500000),
            name="decoder_layers",
        )
        results = call(lengths, ln_attn_g, ln_attn_b, ln_mlp_g, ln_mlp_b, hidden_in[0], w_qkv, w_out, w_up, w_down, cos, sin)
        h_out, kc, vc = pl.pallas_call(
            copy_out,
            out_shape=tuple(jax.ShapeDtypeStruct(r.shape, r.dtype) for r in results),
            in_specs=[hbm] * 3,
            out_specs=(hbm,) * 3,
            scratch_shapes=[dma((3,))],
            compiler_params=pltpu.CompilerParams(vmem_limit_bytes=1 << 20),
            name="copy_out",
        )(*results)
        return h_out[None], kc[:, None], vc[:, None]

    return jax.shard_map(per_device, mesh=mesh, in_specs=(batch_spec, batch_spec) + (weight_spec,) * 8, out_specs=(batch_spec, cache_spec, cache_spec), check_vma=False)
```

```python
import jax
import jax.numpy as jnp
import numpy as np
from jax import lax
from jax.experimental import pallas as pl
from jax.experimental.pallas import tpu as pltpu
from jax.sharding import PartitionSpec as P

MESH = pl.DeviceIdType.MESH
LN_EPS = 1e-5
ROPE_BASE = 10000.0
T = 192
D = 2048
HD = 256
ROWS = 256
QC = 1024
FC = 2048
DR = 1024
HALF = D // 2
UNROLL = 2
RAW = 32
CH = 16
TN = 256
F32 = jnp.float32
BF16 = jnp.bfloat16
PACK, QKV0, UP0, QKV1, UP1 = range(5)


def kernel(len_ref, ga_ref, ba_ref, gm_ref, bm_ref, h_in, wqkv, wout, wup, wdown, cos_hbm, sin_hbm,
           h_out, kc, vc,
           cos_ref, sin_ref, pack, raw, packg, wq, wu, wo, wd, hg, part, rsd, rsb, nb, qkv, ctx, kr, vr,
           ici_s, ici_r, d2d_s, d2d_r, loc, own_s, own_r, own_l,
           raw_l, h_s, h_r, hf_s, hf_r, h_l, rs_s, rs_r, kv_s, kv_r, kv_l, const_l, free):
    me = lax.axis_index("fsdp")
    core = me % 2
    chip = me // 2
    partner = chip * 2 + (1 - core)

    def chip_at(s):
        return ((chip // 2 + s // 2) % 2) * 2 + (chip % 2 + s % 2) % 2

    def peer(s):
        return chip_at(s) * 2 + core

    def remote(src, dst, send, recv, device):
        return pltpu.make_async_remote_copy(
            src_ref=src, dst_ref=dst, send_sem=send, recv_sem=recv,
            device_id={"fsdp": device}, device_id_type=MESH)

    def cols(c, width):
        return pl.ds(pl.multiple_of(c * width, width), width)

    def source(kind, c):
        if kind == PACK:
            return pack
        if kind in (QKV0, QKV1):
            return wd.at[1, pl.ds(pl.multiple_of(core * DR + int(kind == QKV1) * 2 * ROWS + (c // 2) * ROWS, ROWS), ROWS), cols(c % 2, QC)]
        return wup.at[int(kind == UP1), :, cols(c, FC)]

    def landing(kind, row):
        if kind == PACK:
            return packg.at[:, cols(row, ROWS)]
        if kind in (QKV0, QKV1):
            return wq.at[cols(row, ROWS), :]
        return wu.at[int(kind == UP1), cols(row, ROWS), :]

    def ici(kind, s):
        return remote(source(kind, chip_at(s)), landing(kind, me), ici_s.at[kind, s], ici_r.at[kind, s], peer(s))

    def ici_in(kind, s):
        return remote(source(kind, chip), landing(kind, peer(s)), ici_s.at[kind, s], ici_r.at[kind, s], peer(s))

    def d2d(kind, s):
        src = source(kind, chip) if s == 0 else landing(kind, peer(s))
        row = me if s == 0 else peer(s)
        return remote(src, landing(kind, row), d2d_s.at[kind, s], d2d_r.at[kind, s], partner)

    def d2d_in(kind, s):
        row = chip_at(s) * 2 + (1 - core)
        return remote(landing(kind, row), landing(kind, row), d2d_s.at[kind, s], d2d_r.at[kind, s], partner)

    def local(kind):
        return pltpu.make_async_copy(source(kind, chip), landing(kind, me), loc.at[kind])

    def own_refs(layer, which, core_index):
        if which == 0:
            return wout.at[layer], wo.at[layer, cols(core_index, ROWS), :]
        return wdown.at[layer], wd.at[layer, cols(core_index, DR), :]

    def own_remote(layer, which, core_index):
        src, dst = own_refs(layer, which, core_index)
        return remote(src, dst, own_s.at[layer, which], own_r.at[layer, which], partner)

    def own_local(layer, which):
        src, dst = own_refs(layer, which, core)
        return pltpu.make_async_copy(src, dst, own_l.at[layer, which])

    def raw_copy(layer, n, slot):
        return pltpu.make_async_copy(wqkv.at[layer, pl.ds(n * RAW, RAW)], raw.at[slot], raw_l.at[slot])

    def flatten_qkv(layer):
        raw_copy(layer, 0, 0).start()

        def step(n, carry):
            slot = n % 2

            @pl.when(n + 1 < ROWS // RAW)
            def _():
                raw_copy(layer, n + 1, 1 - slot).start()

            raw_copy(layer, n, slot).wait()
            for group in range(4):
                first = core * DR + layer * 2 * ROWS + (group // 2) * ROWS
                rows = pl.ds(pl.multiple_of(first + n * RAW, RAW), RAW)
                for part_of in range(4):
                    at = (group % 2) * QC + part_of * HD
                    wd[1, rows, at:at + HD] = raw[slot, :, group, part_of, :]
            return carry

        lax.fori_loop(0, ROWS // RAW, step, 0)

    def send_block(kind, peers=(3, 1, 2)):
        for s in peers:
            ici(kind, s).start()

    def own_block(kind):
        local(kind).start()
        d2d(kind, 0).start()

    def own_rows(layer):
        for which in range(2):
            own_local(layer, which).start()
            own_remote(layer, which, core).start()

    def relay_block(kind, then=None):
        for n, s in enumerate((3, 1, 2)):
            ici_in(kind, s).wait_recv()
            d2d(kind, s).start()
            if then is not None and n == 0:
                then()

    def block_ready(kind):
        local(kind).wait()
        for s in range(4):
            d2d_in(kind, s).wait_recv()

    def own_ready(layer):
        for which in range(2):
            own_local(layer, which).wait()
            own_remote(layer, which, 1 - core).wait_recv()

    def h_half(j, half):
        return hg.at[j, :, cols(half, HALF)]

    def h_copy(layer, s, half):
        src = h_in.at[:, cols(half, HALF)] if layer == 0 else h_half(chip, half)
        return remote(src, h_half(chip, half), h_s.at[layer, s, half], h_r.at[layer, s, half], peer(s))

    def h_copy_in(layer, s, half):
        dst = h_half(chip_at(s), half)
        return remote(dst, dst, h_s.at[layer, s, half], h_r.at[layer, s, half], peer(s))

    def h_forward(layer, half):
        dst = h_half(chip_at(1 + half), half)
        return remote(dst, dst, hf_s.at[layer, half], hf_r.at[layer, half], peer(2 - half))

    def h_forward_in(layer, half):
        dst = h_half(chip_at(3), half)
        return remote(dst, dst, hf_s.at[layer, half], hf_r.at[layer, half], peer(2 - half))

    def h_send(layer):
        for s, half in ((1, 0), (2, 1), (1, 1), (2, 0)):
            h_copy(layer, s, half).start()

    def h_relay(layer):
        for half in range(2):
            h_copy_in(layer, 1 + half, half).wait_recv()
            h_forward(layer, half).start()

    def h_forwarded(layer):
        for half in range(2):
            h_forward(layer, half).wait_send()

    def h_ready(layer):
        h_forwarded(layer)
        for half in range(2):
            h_copy_in(layer, 2 - half, half).wait_recv()
        for half in range(2):
            h_forward_in(layer, half).wait_recv()

    def h_sent(layer):
        for half in range(2):
            for s in (1, 2):
                h_copy(layer, s, half).wait_send()

    def rs_copy(layer, n):
        s, half, to, dst = (
            (3, 0, 1, rsd.at[0]), (3, 1, 2, rsd.at[1]),
            (1, 0, 1, rsb.at[0]), (2, 1, 2, rsb.at[1]),
            (2, 0, 2, rsb.at[2]), (1, 1, 1, rsb.at[3]))[n]
        return remote(part.at[chip_at(s), half], dst, rs_s.at[layer, n], rs_r.at[layer, n], peer(to))

    def rs_pass_on(layer):
        for half in range(2):
            s = 2 - half
            rs_copy(layer, half).wait_recv()

            def step(i, carry):
                rows = pl.ds(pl.multiple_of(i * CH, CH), CH)
                part[chip_at(s), half, rows, :] = part[chip_at(s), half, rows, :] + rsd[half, rows, :]
                return carry

            lax.fori_loop(0, T // CH, step, 0)
            rs_copy(layer, 4 + half).start()

    def kv_copy(layer, which, s):
        src = (kr, vr)[which].at[layer, chip_at(s)]
        dst = (kc, vc)[which].at[layer, chip]
        return remote(src, dst, kv_s.at[layer, which, s], kv_r.at[layer, which, s], peer(s))

    def kv_copy_in(layer, which, s):
        dst = (kc, vc)[which].at[layer, chip_at(s)]
        return remote(dst, dst, kv_s.at[layer, which, s], kv_r.at[layer, which, s], peer(s))

    def kv_send(layer, parts=(0, 1)):
        for which in parts:
            (kc, vc)[which][layer, chip] = (kr, vr)[which][layer, chip]
            for s in (3, 1, 2):
                kv_copy(layer, which, s).start()

    def kv_sent(layer):
        for which in range(2):
            for s in (3, 1, 2):
                kv_copy(layer, which, s).wait_send()

    def hm_slot(s):
        own = 1 - (s + 3) // 4
        return own * 4 + (1 - own) * chip_at(s)

    def norm(layer, s):
        gain_a, bias_a, gain_m, bias_m = (packg[2 * n + layer:2 * n + layer + 1, :] for n in range(4))

        def step(i, carry):
            rows = pl.ds(pl.multiple_of(i * CH, CH), CH)
            x = hg[chip_at(s), rows, :].astype(F32)
            mean = jnp.sum(x, axis=-1, keepdims=True) * (1.0 / D)
            x = x - mean
            var = jnp.sum(x * x, axis=-1, keepdims=True) * (1.0 / D)
            x = x * lax.rsqrt(var + LN_EPS)
            nb[rows, :] = (x * gain_a + bias_a).astype(BF16)
            hg[hm_slot(s), rows, :] = (x * gain_m + bias_m).astype(BF16)
            return carry

        lax.fori_loop(0, T // CH, step, 0, unroll=UNROLL)

    def rope(u):
        u = u.astype(F32)
        lo, hi = u[:, :HD // 2], u[:, HD // 2:]
        cos, sin = cos_ref[...], sin_ref[...]
        return jnp.concatenate([lo * cos - hi * sin, hi * cos + lo * sin], axis=-1).astype(BF16)

    def attention(layer, s):
        j = chip_at(s)
        norm(layer, s)

        def project(i, carry):
            n = cols(i, TN)
            qkv[:, n] = jnp.dot(nb[...], wq[:, n], preferred_element_type=F32).astype(BF16)
            return carry

        lax.fori_loop(0, QC // TN, project, 0)
        key = rope(qkv[:, 2 * HD:3 * HD])
        kr[layer, j] = key
        vr[layer, j] = qkv[:, 3 * HD:4 * HD]
        length = packg[8:9, pl.ds(pl.multiple_of((j * 2 + core) * ROWS, ROWS), 128)][:, 0:1]
        query_pos = lax.broadcasted_iota(jnp.int32, (T, T), 0)
        key_pos = lax.broadcasted_iota(jnp.int32, (T, T), 1)
        allowed = (key_pos <= query_pos) & (key_pos.astype(F32) < length)
        for head in range(2):
            query = rope(qkv[:, head * HD:(head + 1) * HD])
            scores = lax.dot_general(query, key, (((1,), (1,)), ((), ())), preferred_element_type=F32) * (HD ** -0.5)
            scores = jnp.where(allowed, scores, -1e30)
            expo = jnp.exp(scores - jnp.max(scores, axis=-1, keepdims=True))
            prob = (expo / jnp.sum(expo, axis=-1, keepdims=True)).astype(BF16)
            ctx[j, :, head * HD:(head + 1) * HD] = jnp.dot(prob, vr[layer, j], preferred_element_type=F32).astype(BF16)

    def mlp(layer, s):
        j = chip_at(s)
        hm = hg.at[hm_slot(s)]

        def up(i, carry):
            n = cols(i, TN)
            u = jnp.dot(hm[...], wu[layer, :, n], preferred_element_type=F32)
            nb[:, n] = (0.5 * u * (1.0 + lax.erf(u * np.float32(np.sqrt(0.5))))).astype(BF16)
            return carry

        lax.fori_loop(0, FC // TN, up, 0)

        def down(i, carry):
            n = cols(i, TN)
            acc = jnp.dot(nb[...], wd[layer, :, n], preferred_element_type=F32)
            acc = acc + jnp.dot(ctx[j], wo[layer, :, n], preferred_element_type=F32)
            part[j, i // (HALF // TN), :, cols(i % (HALF // TN), TN)] = acc
            return carry

        for half, sends in ((0, ((0, 3), (2, 1))), (1, ((1, 3), (3, 2)))):
            lax.fori_loop(half * (HALF // TN), (half + 1) * (HALF // TN), down, 0)
            for n, at in sends:
                @pl.when(s == at)
                def _():
                    rs_copy(layer, n).start()

    def residual(layer):
        for half in range(2):
            rs_copy(layer, 2 + half).wait_recv()
        if layer == 0:
            kv_send(0, (0,))

        def direct(i, carry):
            rows = pl.ds(pl.multiple_of(i * CH, CH), CH)
            for half in range(2):
                total = hg[chip, rows, cols(half, HALF)].astype(F32) + part[chip, half, rows, :]
                part[chip, half, rows, :] = total + rsb[half, rows, :]
            return carry

        lax.fori_loop(0, T // CH, direct, 0)
        for half in range(2):
            rs_copy(layer, 4 + half).wait_recv()

        def step(i, carry):
            rows = pl.ds(pl.multiple_of(i * CH, CH), CH)
            for half in range(2):
                total = (part[chip, half, rows, :] + rsb[2 + half, rows, :]).astype(BF16)
                if layer == 0:
                    hg[chip, rows, cols(half, HALF)] = total
                else:
                    h_out[rows, half * HALF:(half + 1) * HALF] = total
            return carry

        lax.fori_loop(0, T // CH, step, 0)

    def qkv_sent():
        for kind in (QKV0, QKV1):
            for s in (3, 1, 2):
                ici(kind, s).wait_send()
        d2d(QKV1, 0).wait_send()

    def attend_all(layer, first):
        def step(s, carry):
            attention(layer, s)
            return carry

        lax.fori_loop(first, 4, step, 0)

    def mlp_all(layer):
        def step(i, carry):
            mlp(layer, 3 - i)
            return carry

        lax.fori_loop(0, 4, step, 0)

    barrier = pltpu.get_barrier_semaphore()
    for s in (1, 2, 3):
        pl.semaphore_signal(barrier, inc=1, device_id={"fsdp": peer(s)}, device_id_type=MESH)
    pl.semaphore_signal(barrier, inc=1, device_id={"fsdp": partner}, device_id_type=MESH)
    pl.semaphore_wait(barrier, 4)

    h_send(0)
    h_local = pltpu.make_async_copy(h_in, hg.at[chip], h_l.at[0])
    h_local.start()
    tables = [pltpu.make_async_copy(src, dst, const_l.at[n])
              for n, (src, dst) in enumerate(((cos_hbm, cos_ref), (sin_hbm, sin_ref)))]
    for table in tables:
        table.start()
    for n, ref in enumerate((ga_ref, ba_ref, gm_ref, bm_ref)):
        pack[2 * n:2 * n + 2, :] = ref[...]
    pack[8:16, :] = jnp.full((8, ROWS), len_ref[0].astype(F32), F32)
    flatten_qkv(0)
    send_block(PACK)
    own_block(PACK)
    send_block(QKV0)
    own_block(QKV0)
    own_block(UP0)
    own_rows(0)
    flatten_qkv(1)
    relay_block(PACK)
    block_ready(PACK)
    h_relay(0)
    relay_block(QKV0, lambda: send_block(UP0))
    h_local.wait()
    for table in tables:
        table.wait()
    h_ready(0)
    block_ready(QKV0)
    attend_all(0, 0)
    for s in range(4):
        d2d(QKV0, s).wait_send()
    for device in (peer(1), peer(2), peer(3), partner):
        pl.semaphore_signal(free, inc=1, device_id={"fsdp": device}, device_id_type=MESH)
    pl.semaphore_wait(free, 4)
    own_block(QKV1)
    own_block(UP1)
    relay_block(UP0, lambda: send_block(QKV1))
    block_ready(UP0)
    own_ready(0)
    mlp_all(0)
    rs_pass_on(0)
    relay_block(QKV1)
    block_ready(QKV1)
    h_sent(0)
    residual(0)
    h_send(1)
    qkv_sent()
    own_rows(1)
    attention(1, 0)
    send_block(UP1, (3,))
    h_relay(1)
    send_block(UP1, (1, 2))
    h_ready(1)
    attend_all(1, 1)

    def rest_of_kv():
        kv_send(0, (1,))
        kv_send(1)

    relay_block(UP1, rest_of_kv)
    block_ready(UP1)
    own_ready(1)
    for n in range(6):
        rs_copy(0, n).wait_send()
    mlp_all(1)
    rs_pass_on(1)
    h_sent(1)
    residual(1)

    for kind in range(5):
        for s in range(4):
            if kind not in (QKV0, QKV1):
                if s > 0:
                    ici(kind, s).wait_send()
                d2d(kind, s).wait_send()
            elif kind == QKV1 and s > 0:
                d2d(kind, s).wait_send()
    for layer in range(2):
        for which in range(2):
            own_remote(layer, which, core).wait_send()
    for n in range(6):
        rs_copy(1, n).wait_send()
    kv_sent(0)
    kv_sent(1)
    for layer in range(2):
        for which in range(2):
            for s in (3, 1, 2):
                kv_copy_in(layer, which, s).wait_recv()


def copy_out(h_in, k_in, v_in, h_out, k_out, v_out, sem):
    pairs = ((h_in, h_out), (k_in, k_out), (v_in, v_out))
    writes = [pltpu.make_async_copy(src, dst, sem.at[n]) for n, (src, dst) in enumerate(pairs)]
    for write in writes:
        write.start()
    for write in writes:
        write.wait()


def rope_tables():
    half = HD // 2
    inv_freq = np.float32(ROPE_BASE) ** (np.float32(-2.0) * np.arange(half, dtype=np.float32) / np.float32(HD))
    angles = np.arange(T, dtype=np.float32)[:, None] * inv_freq.astype(np.float32)[None, :]
    return np.cos(angles).astype(np.float32), np.sin(angles).astype(np.float32)


def solution(mesh):
    batch_spec = P(("dp", "fsdp"))
    weight_spec = P(None, "fsdp")
    cache_spec = P(None, ("dp", "fsdp"))
    vmem = pl.BlockSpec(memory_space=pltpu.VMEM)
    hbm = pl.BlockSpec(memory_space=pl.ANY)
    dma = pltpu.SemaphoreType.DMA

    def per_device(hidden_in, lengths, ln_attn_g, ln_attn_b, ln_mlp_g, ln_mlp_b, w_qkv, w_out, w_up, w_down):
        cos, sin = rope_tables()
        call = pl.pallas_call(
            kernel,
            out_shape=(
                pltpu.VMEM((T, D), BF16),
                pltpu.VMEM((2, 4, T, HD), BF16),
                pltpu.VMEM((2, 4, T, HD), BF16),
            ),
            in_specs=[pl.BlockSpec(memory_space=pltpu.SMEM)] + [vmem] * 4 + [hbm] * 7,
            out_specs=(vmem, vmem, vmem),
            scratch_shapes=[
                pltpu.VMEM((T, HD // 2), F32),
                pltpu.VMEM((T, HD // 2), F32),
                pltpu.VMEM((16, ROWS), F32),
                pltpu.VMEM((2, RAW, 4, 4, HD), BF16),
                pltpu.VMEM((16, D), F32),
                pltpu.VMEM((D, QC), BF16),
                pltpu.VMEM((2, D, FC), BF16),
                pltpu.VMEM((2, 2 * ROWS, D), BF16),
                pltpu.VMEM((2, 2 * DR, D), BF16),
                pltpu.VMEM((5, T, D), BF16),
                pltpu.VMEM((4, 2, T, HALF), F32),
                pltpu.VMEM((2, T, HALF), F32),
                pltpu.VMEM((4, T, HALF), F32),
                pltpu.VMEM((T, D), BF16),
                pltpu.VMEM((T, QC), BF16),
                pltpu.VMEM((4, T, 2 * HD), BF16),
                pltpu.VMEM((2, 4, T, HD), BF16),
                pltpu.VMEM((2, 4, T, HD), BF16),
                dma((5, 4)), dma((5, 4)), dma((5, 4)), dma((5, 4)), dma((5,)),
                dma((2, 2)), dma((2, 2)), dma((2, 2)),
                dma((2,)), dma((2, 3, 2)), dma((2, 3, 2)), dma((2, 2)), dma((2, 2)), dma((1,)),
                dma((2, 6)), dma((2, 6)),
                dma((2, 2, 4)), dma((2, 2, 4)), dma((2, 2)), dma((2,)),
                pltpu.SemaphoreType.REGULAR,
            ],
            compiler_params=pltpu.CompilerParams(
                collective_id=0, has_side_effects=True, vmem_limit_bytes=64500000),
            name="decoder_layers",
        )
        results = call(lengths, ln_attn_g, ln_attn_b, ln_mlp_g, ln_mlp_b, hidden_in[0], w_qkv, w_out, w_up, w_down, cos, sin)
        h_out, kc, vc = pl.pallas_call(
            copy_out,
            out_shape=tuple(jax.ShapeDtypeStruct(r.shape, r.dtype) for r in results),
            in_specs=[hbm] * 3,
            out_specs=(hbm,) * 3,
            scratch_shapes=[dma((3,))],
            compiler_params=pltpu.CompilerParams(vmem_limit_bytes=1 << 20),
            name="copy_out",
        )(*results)
        return h_out[None], kc[:, None], vc[:, None]

    return jax.shard_map(per_device, mesh=mesh, in_specs=(batch_spec, batch_spec) + (weight_spec,) * 8, out_specs=(batch_spec, cache_spec, cache_spec), check_vma=False)
```

```python
import jax
import jax.numpy as jnp
import numpy as np
from jax import lax
from jax.experimental import pallas as pl
from jax.experimental.pallas import tpu as pltpu
from jax.sharding import PartitionSpec as P

MESH = pl.DeviceIdType.MESH
LN_EPS = 1e-5
ROPE_BASE = 10000.0
T = 192
D = 2048
HD = 256
ROWS = 256
QC = 1024
FC = 2048
DR = 1024
HALF = D // 2
UNROLL = 2
RAW = 32
CH = 16
TN = 256
F32 = jnp.float32
BF16 = jnp.bfloat16
PACK, QKV0, UP0, QKV1, UP1 = range(5)


def kernel(len_ref, ga_hbm, ba_hbm, gm_hbm, bm_hbm, h_in, wqkv, wout, wup, wdown, cos_hbm, sin_hbm,
           h_out, kc, vc,
           vectors, cos_ref, sin_ref, pack, raw, packg, wq, wu, wo, wd, hg, part, rsd, rsb, nb, qkv, ctx, kr, vr,
           ici_s, ici_r, d2d_s, d2d_r, loc, own_s, own_r, own_l,
           raw_l, h_s, h_r, hf_s, hf_r, h_l, rs_s, rs_r, kv_s, kv_r, kv_l, const_l, small_l, free):
    me = lax.axis_index("fsdp")
    core = me % 2
    chip = me // 2
    partner = chip * 2 + (1 - core)

    def chip_at(s):
        return ((chip // 2 + s // 2) % 2) * 2 + (chip % 2 + s % 2) % 2

    def peer(s):
        return chip_at(s) * 2 + core

    def remote(src, dst, send, recv, device):
        return pltpu.make_async_remote_copy(
            src_ref=src, dst_ref=dst, send_sem=send, recv_sem=recv,
            device_id={"fsdp": device}, device_id_type=MESH)

    def cols(c, width):
        return pl.ds(pl.multiple_of(c * width, width), width)

    def source(kind, c):
        if kind == PACK:
            return pack
        if kind in (QKV0, QKV1):
            return wd.at[1, pl.ds(pl.multiple_of(core * DR + int(kind == QKV1) * 2 * ROWS + (c // 2) * ROWS, ROWS), ROWS), cols(c % 2, QC)]
        return wup.at[int(kind == UP1), :, cols(c, FC)]

    def landing(kind, row):
        if kind == PACK:
            return packg.at[:, cols(row, ROWS)]
        if kind in (QKV0, QKV1):
            return wq.at[cols(row, ROWS), :]
        return wu.at[int(kind == UP1), cols(row, ROWS), :]

    def ici(kind, s):
        return remote(source(kind, chip_at(s)), landing(kind, me), ici_s.at[kind, s], ici_r.at[kind, s], peer(s))

    def ici_in(kind, s):
        return remote(source(kind, chip), landing(kind, peer(s)), ici_s.at[kind, s], ici_r.at[kind, s], peer(s))

    def d2d(kind, s):
        src = source(kind, chip) if s == 0 else landing(kind, peer(s))
        row = me if s == 0 else peer(s)
        return remote(src, landing(kind, row), d2d_s.at[kind, s], d2d_r.at[kind, s], partner)

    def d2d_in(kind, s):
        row = chip_at(s) * 2 + (1 - core)
        return remote(landing(kind, row), landing(kind, row), d2d_s.at[kind, s], d2d_r.at[kind, s], partner)

    def local(kind):
        return pltpu.make_async_copy(source(kind, chip), landing(kind, me), loc.at[kind])

    def own_refs(layer, which, core_index):
        if which == 0:
            return wout.at[layer], wo.at[layer, cols(core_index, ROWS), :]
        return wdown.at[layer], wd.at[layer, cols(core_index, DR), :]

    def own_remote(layer, which, core_index):
        src, dst = own_refs(layer, which, core_index)
        return remote(src, dst, own_s.at[layer, which], own_r.at[layer, which], partner)

    def own_local(layer, which):
        src, dst = own_refs(layer, which, core)
        return pltpu.make_async_copy(src, dst, own_l.at[layer, which])

    def raw_copy(layer, n, slot):
        return pltpu.make_async_copy(wqkv.at[layer, pl.ds(n * RAW, RAW)], raw.at[slot], raw_l.at[slot])

    def flatten_qkv(layer):
        raw_copy(layer, 0, 0).start()

        def step(n, carry):
            slot = n % 2

            @pl.when(n + 1 < ROWS // RAW)
            def _():
                raw_copy(layer, n + 1, 1 - slot).start()

            raw_copy(layer, n, slot).wait()
            for group in range(4):
                first = core * DR + layer * 2 * ROWS + (group // 2) * ROWS
                rows = pl.ds(pl.multiple_of(first + n * RAW, RAW), RAW)
                for part_of in range(4):
                    at = (group % 2) * QC + part_of * HD
                    wd[1, rows, at:at + HD] = raw[slot, :, group, part_of, :]
            return carry

        lax.fori_loop(0, ROWS // RAW, step, 0)

    def send_block(kind, peers=(3, 1, 2)):
        for s in peers:
            ici(kind, s).start()

    def own_block(kind):
        local(kind).start()
        d2d(kind, 0).start()

    def own_rows(layer):
        for which in range(2):
            own_local(layer, which).start()
            own_remote(layer, which, core).start()

    def relay_block(kind, then=None):
        for n, s in enumerate((3, 1, 2)):
            ici_in(kind, s).wait_recv()
            d2d(kind, s).start()
            if then is not None and n == 0:
                then()

    def block_ready(kind):
        local(kind).wait()
        for s in range(4):
            d2d_in(kind, s).wait_recv()

    def own_ready(layer):
        for which in range(2):
            own_local(layer, which).wait()
            own_remote(layer, which, 1 - core).wait_recv()

    def h_half(j, half):
        return hg.at[j, :, cols(half, HALF)]

    def h_copy(layer, s, half):
        src = h_in.at[:, cols(half, HALF)] if layer == 0 else h_half(chip, half)
        return remote(src, h_half(chip, half), h_s.at[layer, s, half], h_r.at[layer, s, half], peer(s))

    def h_copy_in(layer, s, half):
        dst = h_half(chip_at(s), half)
        return remote(dst, dst, h_s.at[layer, s, half], h_r.at[layer, s, half], peer(s))

    def h_forward(layer, half):
        dst = h_half(chip_at(1 + half), half)
        return remote(dst, dst, hf_s.at[layer, half], hf_r.at[layer, half], peer(2 - half))

    def h_forward_in(layer, half):
        dst = h_half(chip_at(3), half)
        return remote(dst, dst, hf_s.at[layer, half], hf_r.at[layer, half], peer(2 - half))

    def h_send(layer):
        for s, half in ((1, 0), (2, 1), (1, 1), (2, 0)):
            h_copy(layer, s, half).start()

    def h_relay(layer):
        for half in range(2):
            h_copy_in(layer, 1 + half, half).wait_recv()
            h_forward(layer, half).start()

    def h_forwarded(layer):
        for half in range(2):
            h_forward(layer, half).wait_send()

    def h_ready(layer):
        h_forwarded(layer)
        for half in range(2):
            h_copy_in(layer, 2 - half, half).wait_recv()
        for half in range(2):
            h_forward_in(layer, half).wait_recv()

    def h_sent(layer):
        for half in range(2):
            for s in (1, 2):
                h_copy(layer, s, half).wait_send()

    def rs_copy(layer, n):
        s, half, to, dst = (
            (3, 0, 1, rsd.at[0]), (3, 1, 2, rsd.at[1]),
            (1, 0, 1, rsb.at[0]), (2, 1, 2, rsb.at[1]),
            (2, 0, 2, rsb.at[2]), (1, 1, 1, rsb.at[3]))[n]
        return remote(part.at[chip_at(s), half], dst, rs_s.at[layer, n], rs_r.at[layer, n], peer(to))

    def rs_pass_on(layer):
        for half in range(2):
            s = 2 - half
            rs_copy(layer, half).wait_recv()

            def step(i, carry):
                rows = pl.ds(pl.multiple_of(i * CH, CH), CH)
                part[chip_at(s), half, rows, :] = part[chip_at(s), half, rows, :] + rsd[half, rows, :]
                return carry

            lax.fori_loop(0, T // CH, step, 0)
            rs_copy(layer, 4 + half).start()

    def kv_copy(layer, which, s):
        src = (kr, vr)[which].at[layer, chip_at(s)]
        dst = (kc, vc)[which].at[layer, chip]
        return remote(src, dst, kv_s.at[layer, which, s], kv_r.at[layer, which, s], peer(s))

    def kv_copy_in(layer, which, s):
        dst = (kc, vc)[which].at[layer, chip_at(s)]
        return remote(dst, dst, kv_s.at[layer, which, s], kv_r.at[layer, which, s], peer(s))

    def kv_send(layer, parts=(0, 1)):
        for which in parts:
            (kc, vc)[which][layer, chip] = (kr, vr)[which][layer, chip]
            for s in (3, 1, 2):
                kv_copy(layer, which, s).start()

    def kv_sent(layer):
        for which in range(2):
            for s in (3, 1, 2):
                kv_copy(layer, which, s).wait_send()

    def hm_slot(s):
        own = 1 - (s + 3) // 4
        return own * 4 + (1 - own) * chip_at(s)

    def norm(layer, s):
        gain_a, bias_a, gain_m, bias_m = (packg[2 * n + layer:2 * n + layer + 1, :] for n in range(4))

        def step(i, carry):
            rows = pl.ds(pl.multiple_of(i * CH, CH), CH)
            x = hg[chip_at(s), rows, :].astype(F32)
            mean = jnp.sum(x, axis=-1, keepdims=True) * (1.0 / D)
            x = x - mean
            var = jnp.sum(x * x, axis=-1, keepdims=True) * (1.0 / D)
            x = x * lax.rsqrt(var + LN_EPS)
            nb[rows, :] = (x * gain_a + bias_a).astype(BF16)
            hg[hm_slot(s), rows, :] = (x * gain_m + bias_m).astype(BF16)
            return carry

        lax.fori_loop(0, T // CH, step, 0, unroll=UNROLL)

    def rope(u):
        u = u.astype(F32)
        lo, hi = u[:, :HD // 2], u[:, HD // 2:]
        cos, sin = cos_ref[...], sin_ref[...]
        return jnp.concatenate([lo * cos - hi * sin, hi * cos + lo * sin], axis=-1).astype(BF16)

    def attention(layer, s):
        j = chip_at(s)
        norm(layer, s)

        def project(i, carry):
            n = cols(i, TN)
            qkv[:, n] = jnp.dot(nb[...], wq[:, n], preferred_element_type=F32).astype(BF16)
            return carry

        lax.fori_loop(0, QC // TN, project, 0)
        key = rope(qkv[:, 2 * HD:3 * HD])
        kr[layer, j] = key
        vr[layer, j] = qkv[:, 3 * HD:4 * HD]
        length = packg[8:9, pl.ds(pl.multiple_of((j * 2 + core) * ROWS, ROWS), 128)][:, 0:1]
        query_pos = lax.broadcasted_iota(jnp.int32, (T, T), 0)
        key_pos = lax.broadcasted_iota(jnp.int32, (T, T), 1)
        allowed = (key_pos <= query_pos) & (key_pos.astype(F32) < length)
        for head in range(2):
            query = rope(qkv[:, head * HD:(head + 1) * HD])
            scores = lax.dot_general(query, key, (((1,), (1,)), ((), ())), preferred_element_type=F32) * (HD ** -0.5)
            scores = jnp.where(allowed, scores, -1e30)
            expo = jnp.exp(scores - jnp.max(scores, axis=-1, keepdims=True))
            prob = (expo / jnp.sum(expo, axis=-1, keepdims=True)).astype(BF16)
            ctx[j, :, head * HD:(head + 1) * HD] = jnp.dot(prob, vr[layer, j], preferred_element_type=F32).astype(BF16)

    def mlp(layer, s):
        j = chip_at(s)
        hm = hg.at[hm_slot(s)]

        def up(i, carry):
            n = cols(i, TN)
            u = jnp.dot(hm[...], wu[layer, :, n], preferred_element_type=F32)
            nb[:, n] = (0.5 * u * (1.0 + lax.erf(u * np.float32(np.sqrt(0.5))))).astype(BF16)
            return carry

        lax.fori_loop(0, FC // TN, up, 0)

        def down(i, carry):
            n = cols(i, TN)
            acc = jnp.dot(nb[...], wd[layer, :, n], preferred_element_type=F32)
            acc = acc + jnp.dot(ctx[j], wo[layer, :, n], preferred_element_type=F32)
            part[j, i // (HALF // TN), :, cols(i % (HALF // TN), TN)] = acc
            return carry

        for half, sends in ((0, ((0, 3), (2, 1))), (1, ((1, 3), (3, 2)))):
            lax.fori_loop(half * (HALF // TN), (half + 1) * (HALF // TN), down, 0)
            for n, at in sends:
                @pl.when(s == at)
                def _():
                    rs_copy(layer, n).start()

    def residual(layer):
        for half in range(2):
            rs_copy(layer, 2 + half).wait_recv()
        if layer == 0:
            kv_send(0, (0,))

        def direct(i, carry):
            rows = pl.ds(pl.multiple_of(i * CH, CH), CH)
            for half in range(2):
                total = hg[chip, rows, cols(half, HALF)].astype(F32) + part[chip, half, rows, :]
                part[chip, half, rows, :] = total + rsb[half, rows, :]
            return carry

        lax.fori_loop(0, T // CH, direct, 0)
        for half in range(2):
            rs_copy(layer, 4 + half).wait_recv()

        def step(i, carry):
            rows = pl.ds(pl.multiple_of(i * CH, CH), CH)
            for half in range(2):
                total = (part[chip, half, rows, :] + rsb[2 + half, rows, :]).astype(BF16)
                if layer == 0:
                    hg[chip, rows, cols(half, HALF)] = total
                else:
                    h_out[rows, half * HALF:(half + 1) * HALF] = total
            return carry

        lax.fori_loop(0, T // CH, step, 0)

    def qkv_sent():
        for kind in (QKV0, QKV1):
            for s in (3, 1, 2):
                ici(kind, s).wait_send()
        d2d(QKV1, 0).wait_send()

    def attend_all(layer, first):
        def step(s, carry):
            attention(layer, s)
            return carry

        lax.fori_loop(first, 4, step, 0)

    def mlp_all(layer):
        def step(i, carry):
            mlp(layer, 3 - i)
            return carry

        lax.fori_loop(0, 4, step, 0)

    small = [pltpu.make_async_copy(src, vectors.at[n], small_l.at[n])
             for n, src in enumerate((ga_hbm, ba_hbm, gm_hbm, bm_hbm))]
    for copy in small:
        copy.start()
    barrier = pltpu.get_barrier_semaphore()
    for s in (1, 2, 3):
        pl.semaphore_signal(barrier, inc=1, device_id={"fsdp": peer(s)}, device_id_type=MESH)
    pl.semaphore_signal(barrier, inc=1, device_id={"fsdp": partner}, device_id_type=MESH)
    pl.semaphore_wait(barrier, 4)

    h_send(0)
    h_local = pltpu.make_async_copy(h_in, hg.at[chip], h_l.at[0])
    h_local.start()
    tables = [pltpu.make_async_copy(src, dst, const_l.at[n])
              for n, (src, dst) in enumerate(((cos_hbm, cos_ref), (sin_hbm, sin_ref)))]
    for table in tables:
        table.start()
    for copy in small:
        copy.wait()
    for n in range(4):
        pack[2 * n:2 * n + 2, :] = vectors[n]
    pack[8:16, :] = jnp.full((8, ROWS), len_ref[0].astype(F32), F32)
    flatten_qkv(0)
    send_block(PACK)
    own_block(PACK)
    send_block(QKV0)
    own_block(QKV0)
    own_block(UP0)
    own_rows(0)
    flatten_qkv(1)
    relay_block(PACK)
    block_ready(PACK)
    h_relay(0)
    relay_block(QKV0, lambda: send_block(UP0))
    h_local.wait()
    for table in tables:
        table.wait()
    h_ready(0)
    block_ready(QKV0)
    attend_all(0, 0)
    for s in range(4):
        d2d(QKV0, s).wait_send()
    for device in (peer(1), peer(2), peer(3), partner):
        pl.semaphore_signal(free, inc=1, device_id={"fsdp": device}, device_id_type=MESH)
    pl.semaphore_wait(free, 4)
    own_block(QKV1)
    own_block(UP1)
    relay_block(UP0, lambda: send_block(QKV1))
    block_ready(UP0)
    own_ready(0)
    mlp_all(0)
    rs_pass_on(0)
    relay_block(QKV1)
    block_ready(QKV1)
    h_sent(0)
    residual(0)
    h_send(1)
    qkv_sent()
    own_rows(1)
    attention(1, 0)
    send_block(UP1, (3,))
    h_relay(1)
    send_block(UP1, (1, 2))
    h_ready(1)
    attend_all(1, 1)

    def rest_of_kv():
        kv_send(0, (1,))
        kv_send(1)

    relay_block(UP1, rest_of_kv)
    block_ready(UP1)
    own_ready(1)
    for n in range(6):
        rs_copy(0, n).wait_send()
    mlp_all(1)
    rs_pass_on(1)
    h_sent(1)
    residual(1)

    for kind in range(5):
        for s in range(4):
            if kind not in (QKV0, QKV1):
                if s > 0:
                    ici(kind, s).wait_send()
                d2d(kind, s).wait_send()
            elif kind == QKV1 and s > 0:
                d2d(kind, s).wait_send()
    for layer in range(2):
        for which in range(2):
            own_remote(layer, which, core).wait_send()
    for n in range(6):
        rs_copy(1, n).wait_send()
    kv_sent(0)
    kv_sent(1)
    for layer in range(2):
        for which in range(2):
            for s in (3, 1, 2):
                kv_copy_in(layer, which, s).wait_recv()


def copy_out(h_in, k_in, v_in, h_out, k_out, v_out, sem):
    pairs = ((h_in, h_out), (k_in, k_out), (v_in, v_out))
    writes = [pltpu.make_async_copy(src, dst, sem.at[n]) for n, (src, dst) in enumerate(pairs)]
    for write in writes:
        write.start()
    for write in writes:
        write.wait()


def rope_tables():
    half = HD // 2
    inv_freq = np.float32(ROPE_BASE) ** (np.float32(-2.0) * np.arange(half, dtype=np.float32) / np.float32(HD))
    angles = np.arange(T, dtype=np.float32)[:, None] * inv_freq.astype(np.float32)[None, :]
    return np.cos(angles).astype(np.float32), np.sin(angles).astype(np.float32)


def solution(mesh):
    batch_spec = P(("dp", "fsdp"))
    weight_spec = P(None, "fsdp")
    cache_spec = P(None, ("dp", "fsdp"))
    vmem = pl.BlockSpec(memory_space=pltpu.VMEM)
    hbm = pl.BlockSpec(memory_space=pl.ANY)
    dma = pltpu.SemaphoreType.DMA

    def per_device(hidden_in, lengths, ln_attn_g, ln_attn_b, ln_mlp_g, ln_mlp_b, w_qkv, w_out, w_up, w_down):
        cos, sin = rope_tables()
        call = pl.pallas_call(
            kernel,
            out_shape=(
                pltpu.VMEM((T, D), BF16),
                pltpu.VMEM((2, 4, T, HD), BF16),
                pltpu.VMEM((2, 4, T, HD), BF16),
            ),
            in_specs=[pl.BlockSpec(memory_space=pltpu.SMEM)] + [hbm] * 11,
            out_specs=(vmem, vmem, vmem),
            scratch_shapes=[
                pltpu.VMEM((4, 2, ROWS), F32),
                pltpu.VMEM((T, HD // 2), F32),
                pltpu.VMEM((T, HD // 2), F32),
                pltpu.VMEM((16, ROWS), F32),
                pltpu.VMEM((2, RAW, 4, 4, HD), BF16),
                pltpu.VMEM((16, D), F32),
                pltpu.VMEM((D, QC), BF16),
                pltpu.VMEM((2, D, FC), BF16),
                pltpu.VMEM((2, 2 * ROWS, D), BF16),
                pltpu.VMEM((2, 2 * DR, D), BF16),
                pltpu.VMEM((5, T, D), BF16),
                pltpu.VMEM((4, 2, T, HALF), F32),
                pltpu.VMEM((2, T, HALF), F32),
                pltpu.VMEM((4, T, HALF), F32),
                pltpu.VMEM((T, D), BF16),
                pltpu.VMEM((T, QC), BF16),
                pltpu.VMEM((4, T, 2 * HD), BF16),
                pltpu.VMEM((2, 4, T, HD), BF16),
                pltpu.VMEM((2, 4, T, HD), BF16),
                dma((5, 4)), dma((5, 4)), dma((5, 4)), dma((5, 4)), dma((5,)),
                dma((2, 2)), dma((2, 2)), dma((2, 2)),
                dma((2,)), dma((2, 3, 2)), dma((2, 3, 2)), dma((2, 2)), dma((2, 2)), dma((1,)),
                dma((2, 6)), dma((2, 6)),
                dma((2, 2, 4)), dma((2, 2, 4)), dma((2, 2)), dma((2,)),
                dma((5,)),
                pltpu.SemaphoreType.REGULAR,
            ],
            compiler_params=pltpu.CompilerParams(
                collective_id=0, has_side_effects=True, vmem_limit_bytes=64500000),
            name="decoder_layers",
        )
        results = call(lengths, ln_attn_g, ln_attn_b, ln_mlp_g, ln_mlp_b, hidden_in[0], w_qkv, w_out, w_up, w_down, cos, sin)
        h_out, kc, vc = pl.pallas_call(
            copy_out,
            out_shape=tuple(jax.ShapeDtypeStruct(r.shape, r.dtype) for r in results),
            in_specs=[hbm] * 3,
            out_specs=(hbm,) * 3,
            scratch_shapes=[dma((3,))],
            compiler_params=pltpu.CompilerParams(vmem_limit_bytes=1 << 20),
            name="copy_out",
        )(*results)
        return h_out[None], kc[:, None], vc[:, None]

    return jax.shard_map(per_device, mesh=mesh, in_specs=(batch_spec, batch_spec) + (weight_spec,) * 8, out_specs=(batch_spec, cache_spec, cache_spec), check_vma=False)
```

```python
import jax
import jax.numpy as jnp
import numpy as np
from jax import lax
from jax.experimental import pallas as pl
from jax.experimental.pallas import tpu as pltpu
from jax.sharding import PartitionSpec as P

MESH = pl.DeviceIdType.MESH
LN_EPS = 1e-5
ROPE_BASE = 10000.0
T = 192
D = 2048
HD = 256
ROWS = 256
QC = 1024
FC = 2048
DR = 1024
HALF = D // 2
UNROLL = 2
PW = ROWS + 128
RAW = 32
CH = 16
TN = 256
F32 = jnp.float32
BF16 = jnp.bfloat16
PACK, QKV0, UP0, QKV1, UP1 = range(5)


def kernel(len_ref, ga_hbm, ba_hbm, gm_hbm, bm_hbm, h_in, wqkv, wout, wup, wdown, cos_hbm, sin_hbm,
           h_out, kc, vc,
           vectors, cos_ref, sin_ref, pack, packl, raw, packg, wq, wu, wo, wd, hg, part, rsd, rsb, nb, qkv, ctx, kr, vr,
           ici_s, ici_r, d2d_s, d2d_r, loc, own_s, own_r, own_l,
           raw_l, h_s, h_r, hf_s, hf_r, h_l, rs_s, rs_r, kv_s, kv_r, kv_l, const_l, small_l, free):
    me = lax.axis_index("fsdp")
    core = me % 2
    chip = me // 2
    partner = chip * 2 + (1 - core)

    def chip_at(s):
        return ((chip // 2 + s // 2) % 2) * 2 + (chip % 2 + s % 2) % 2

    def peer(s):
        return chip_at(s) * 2 + core

    def remote(src, dst, send, recv, device):
        return pltpu.make_async_remote_copy(
            src_ref=src, dst_ref=dst, send_sem=send, recv_sem=recv,
            device_id={"fsdp": device}, device_id_type=MESH)

    def cols(c, width):
        return pl.ds(pl.multiple_of(c * width, width), width)

    def source(kind, c):
        if kind == PACK:
            return pack
        if kind in (QKV0, QKV1):
            return wd.at[1, pl.ds(pl.multiple_of(core * DR + int(kind == QKV1) * 2 * ROWS + (c // 2) * ROWS, ROWS), ROWS), cols(c % 2, QC)]
        return wup.at[int(kind == UP1), :, cols(c, FC)]

    def landing(kind, row):
        if kind == PACK:
            return packl.at[row]
        if kind in (QKV0, QKV1):
            return wq.at[cols(row, ROWS), :]
        return wu.at[int(kind == UP1), cols(row, ROWS), :]

    def ici(kind, s):
        return remote(source(kind, chip_at(s)), landing(kind, me), ici_s.at[kind, s], ici_r.at[kind, s], peer(s))

    def ici_in(kind, s):
        return remote(source(kind, chip), landing(kind, peer(s)), ici_s.at[kind, s], ici_r.at[kind, s], peer(s))

    def d2d(kind, s):
        src = source(kind, chip) if s == 0 else landing(kind, peer(s))
        row = me if s == 0 else peer(s)
        return remote(src, landing(kind, row), d2d_s.at[kind, s], d2d_r.at[kind, s], partner)

    def d2d_in(kind, s):
        row = chip_at(s) * 2 + (1 - core)
        return remote(landing(kind, row), landing(kind, row), d2d_s.at[kind, s], d2d_r.at[kind, s], partner)

    def local(kind):
        return pltpu.make_async_copy(source(kind, chip), landing(kind, me), loc.at[kind])

    def own_refs(layer, which, core_index):
        if which == 0:
            return wout.at[layer], wo.at[layer, cols(core_index, ROWS), :]
        return wdown.at[layer], wd.at[layer, cols(core_index, DR), :]

    def own_remote(layer, which, core_index):
        src, dst = own_refs(layer, which, core_index)
        return remote(src, dst, own_s.at[layer, which], own_r.at[layer, which], partner)

    def own_local(layer, which):
        src, dst = own_refs(layer, which, core)
        return pltpu.make_async_copy(src, dst, own_l.at[layer, which])

    def raw_copy(layer, n, slot):
        return pltpu.make_async_copy(wqkv.at[layer, pl.ds(n * RAW, RAW)], raw.at[slot], raw_l.at[slot])

    def flatten_qkv(layer):
        raw_copy(layer, 0, 0).start()

        def step(n, carry):
            slot = n % 2

            @pl.when(n + 1 < ROWS // RAW)
            def _():
                raw_copy(layer, n + 1, 1 - slot).start()

            raw_copy(layer, n, slot).wait()
            for group in range(4):
                first = core * DR + layer * 2 * ROWS + (group // 2) * ROWS
                rows = pl.ds(pl.multiple_of(first + n * RAW, RAW), RAW)
                for part_of in range(4):
                    at = (group % 2) * QC + part_of * HD
                    wd[1, rows, at:at + HD] = raw[slot, :, group, part_of, :]
            return carry

        lax.fori_loop(0, ROWS // RAW, step, 0)

    def send_block(kind, peers=(3, 1, 2)):
        for s in peers:
            ici(kind, s).start()

    def own_block(kind):
        local(kind).start()
        d2d(kind, 0).start()

    def own_rows(layer):
        for which in range(2):
            own_local(layer, which).start()
            own_remote(layer, which, core).start()

    def relay_block(kind, then=None):
        for n, s in enumerate((3, 1, 2)):
            ici_in(kind, s).wait_recv()
            d2d(kind, s).start()
            if then is not None and n == 0:
                then()

    def block_ready(kind):
        local(kind).wait()
        for s in range(4):
            d2d_in(kind, s).wait_recv()

    def own_ready(layer):
        for which in range(2):
            own_local(layer, which).wait()
            own_remote(layer, which, 1 - core).wait_recv()

    def h_half(j, half):
        return hg.at[j, :, cols(half, HALF)]

    def h_copy(layer, s, half):
        src = h_in.at[:, cols(half, HALF)] if layer == 0 else h_half(chip, half)
        return remote(src, h_half(chip, half), h_s.at[layer, s, half], h_r.at[layer, s, half], peer(s))

    def h_copy_in(layer, s, half):
        dst = h_half(chip_at(s), half)
        return remote(dst, dst, h_s.at[layer, s, half], h_r.at[layer, s, half], peer(s))

    def h_forward(layer, half):
        dst = h_half(chip_at(1 + half), half)
        return remote(dst, dst, hf_s.at[layer, half], hf_r.at[layer, half], peer(2 - half))

    def h_forward_in(layer, half):
        dst = h_half(chip_at(3), half)
        return remote(dst, dst, hf_s.at[layer, half], hf_r.at[layer, half], peer(2 - half))

    def h_send(layer):
        for s, half in ((1, 0), (2, 1), (1, 1), (2, 0)):
            h_copy(layer, s, half).start()

    def h_relay(layer):
        for half in range(2):
            h_copy_in(layer, 1 + half, half).wait_recv()
            h_forward(layer, half).start()

    def h_forwarded(layer):
        for half in range(2):
            h_forward(layer, half).wait_send()

    def h_ready(layer):
        h_forwarded(layer)
        for half in range(2):
            h_copy_in(layer, 2 - half, half).wait_recv()
        for half in range(2):
            h_forward_in(layer, half).wait_recv()

    def h_sent(layer):
        for half in range(2):
            for s in (1, 2):
                h_copy(layer, s, half).wait_send()

    def rs_copy(layer, n):
        s, half, to, dst = (
            (3, 0, 1, rsd.at[0]), (3, 1, 2, rsd.at[1]),
            (1, 0, 1, rsb.at[0]), (2, 1, 2, rsb.at[1]),
            (2, 0, 2, rsb.at[2]), (1, 1, 1, rsb.at[3]))[n]
        return remote(part.at[chip_at(s), half], dst, rs_s.at[layer, n], rs_r.at[layer, n], peer(to))

    def rs_pass_on(layer):
        for half in range(2):
            s = 2 - half
            rs_copy(layer, half).wait_recv()

            def step(i, carry):
                rows = pl.ds(pl.multiple_of(i * CH, CH), CH)
                part[chip_at(s), half, rows, :] = part[chip_at(s), half, rows, :] + rsd[half, rows, :]
                return carry

            lax.fori_loop(0, T // CH, step, 0)
            rs_copy(layer, 4 + half).start()

    def kv_copy(layer, which, s):
        src = (kr, vr)[which].at[layer, chip_at(s)]
        dst = (kc, vc)[which].at[layer, chip]
        return remote(src, dst, kv_s.at[layer, which, s], kv_r.at[layer, which, s], peer(s))

    def kv_copy_in(layer, which, s):
        dst = (kc, vc)[which].at[layer, chip_at(s)]
        return remote(dst, dst, kv_s.at[layer, which, s], kv_r.at[layer, which, s], peer(s))

    def kv_send(layer, parts=(0, 1)):
        for which in parts:
            (kc, vc)[which][layer, chip] = (kr, vr)[which][layer, chip]
            for s in (3, 1, 2):
                kv_copy(layer, which, s).start()

    def kv_sent(layer):
        for which in range(2):
            for s in (3, 1, 2):
                kv_copy(layer, which, s).wait_send()

    def hm_slot(s):
        own = 1 - (s + 3) // 4
        return own * 4 + (1 - own) * chip_at(s)

    def norm(layer, s):
        gain_a, bias_a, gain_m, bias_m = (packg[2 * n + layer:2 * n + layer + 1, :] for n in range(4))

        def step(i, carry):
            rows = pl.ds(pl.multiple_of(i * CH, CH), CH)
            x = hg[chip_at(s), rows, :].astype(F32)
            mean = jnp.sum(x, axis=-1, keepdims=True) * (1.0 / D)
            x = x - mean
            var = jnp.sum(x * x, axis=-1, keepdims=True) * (1.0 / D)
            x = x * lax.rsqrt(var + LN_EPS)
            nb[rows, :] = (x * gain_a + bias_a).astype(BF16)
            hg[hm_slot(s), rows, :] = (x * gain_m + bias_m).astype(BF16)
            return carry

        lax.fori_loop(0, T // CH, step, 0, unroll=UNROLL)

    def rope(u):
        u = u.astype(F32)
        lo, hi = u[:, :HD // 2], u[:, HD // 2:]
        cos, sin = cos_ref[...], sin_ref[...]
        return jnp.concatenate([lo * cos - hi * sin, hi * cos + lo * sin], axis=-1).astype(BF16)

    def attention(layer, s):
        j = chip_at(s)
        norm(layer, s)

        def project(i, carry):
            n = cols(i, TN)
            qkv[:, n] = jnp.dot(nb[...], wq[:, n], preferred_element_type=F32).astype(BF16)
            return carry

        lax.fori_loop(0, QC // TN, project, 0)
        key = rope(qkv[:, 2 * HD:3 * HD])
        kr[layer, j] = key
        vr[layer, j] = qkv[:, 3 * HD:4 * HD]
        length = packl[j * 2 + core, 0:1, ROWS:PW][:, 0:1]
        query_pos = lax.broadcasted_iota(jnp.int32, (T, T), 0)
        key_pos = lax.broadcasted_iota(jnp.int32, (T, T), 1)
        allowed = (key_pos <= query_pos) & (key_pos.astype(F32) < length)
        for head in range(2):
            query = rope(qkv[:, head * HD:(head + 1) * HD])
            scores = lax.dot_general(query, key, (((1,), (1,)), ((), ())), preferred_element_type=F32) * (HD ** -0.5)
            scores = jnp.where(allowed, scores, -1e30)
            expo = jnp.exp(scores - jnp.max(scores, axis=-1, keepdims=True))
            prob = (expo / jnp.sum(expo, axis=-1, keepdims=True)).astype(BF16)
            ctx[j, :, head * HD:(head + 1) * HD] = jnp.dot(prob, vr[layer, j], preferred_element_type=F32).astype(BF16)

    def mlp(layer, s):
        j = chip_at(s)
        hm = hg.at[hm_slot(s)]

        def up(i, carry):
            n = cols(i, TN)
            u = jnp.dot(hm[...], wu[layer, :, n], preferred_element_type=F32)
            nb[:, n] = (0.5 * u * (1.0 + lax.erf(u * np.float32(np.sqrt(0.5))))).astype(BF16)
            return carry

        lax.fori_loop(0, FC // TN, up, 0)

        def down(i, carry):
            n = cols(i, TN)
            acc = jnp.dot(nb[...], wd[layer, :, n], preferred_element_type=F32)
            acc = acc + jnp.dot(ctx[j], wo[layer, :, n], preferred_element_type=F32)
            part[j, i // (HALF // TN), :, cols(i % (HALF // TN), TN)] = acc
            return carry

        for half, sends in ((0, ((0, 3), (2, 1))), (1, ((1, 3), (3, 2)))):
            lax.fori_loop(half * (HALF // TN), (half + 1) * (HALF // TN), down, 0)
            for n, at in sends:
                @pl.when(s == at)
                def _():
                    rs_copy(layer, n).start()

    def residual(layer):
        for half in range(2):
            rs_copy(layer, 2 + half).wait_recv()
        if layer == 0:
            kv_send(0, (0,))

        def direct(i, carry):
            rows = pl.ds(pl.multiple_of(i * CH, CH), CH)
            for half in range(2):
                total = hg[chip, rows, cols(half, HALF)].astype(F32) + part[chip, half, rows, :]
                part[chip, half, rows, :] = total + rsb[half, rows, :]
            return carry

        lax.fori_loop(0, T // CH, direct, 0)
        for half in range(2):
            rs_copy(layer, 4 + half).wait_recv()

        def step(i, carry):
            rows = pl.ds(pl.multiple_of(i * CH, CH), CH)
            for half in range(2):
                total = (part[chip, half, rows, :] + rsb[2 + half, rows, :]).astype(BF16)
                if layer == 0:
                    hg[chip, rows, cols(half, HALF)] = total
                else:
                    h_out[rows, half * HALF:(half + 1) * HALF] = total
            return carry

        lax.fori_loop(0, T // CH, step, 0)

    def qkv_sent():
        for kind in (QKV0, QKV1):
            for s in (3, 1, 2):
                ici(kind, s).wait_send()
        d2d(QKV1, 0).wait_send()

    def attend_all(layer, first):
        def step(s, carry):
            attention(layer, s)
            return carry

        lax.fori_loop(first, 4, step, 0)

    def mlp_all(layer):
        def step(i, carry):
            mlp(layer, 3 - i)
            return carry

        lax.fori_loop(0, 4, step, 0)

    small = [pltpu.make_async_copy(src, vectors.at[n], small_l.at[n])
             for n, src in enumerate((ga_hbm, ba_hbm, gm_hbm, bm_hbm))]
    for copy in small:
        copy.start()
    barrier = pltpu.get_barrier_semaphore()
    for s in (1, 2, 3):
        pl.semaphore_signal(barrier, inc=1, device_id={"fsdp": peer(s)}, device_id_type=MESH)
    pl.semaphore_signal(barrier, inc=1, device_id={"fsdp": partner}, device_id_type=MESH)
    pl.semaphore_wait(barrier, 4)

    h_send(0)
    h_local = pltpu.make_async_copy(h_in, hg.at[chip], h_l.at[0])
    h_local.start()
    tables = [pltpu.make_async_copy(src, dst, const_l.at[n])
              for n, (src, dst) in enumerate(((cos_hbm, cos_ref), (sin_hbm, sin_ref)))]
    for table in tables:
        table.start()
    for copy in small:
        copy.wait()
    for n in range(4):
        pack[2 * n:2 * n + 2, 0:ROWS] = vectors[n]
    pack[:, ROWS:PW] = jnp.full((8, PW - ROWS), len_ref[0].astype(F32), F32)
    flatten_qkv(0)
    send_block(PACK)
    own_block(PACK)
    send_block(QKV0)
    own_block(QKV0)
    own_block(UP0)
    own_rows(0)
    flatten_qkv(1)
    relay_block(PACK)
    block_ready(PACK)
    for n in range(8):
        packg[:, n * ROWS:(n + 1) * ROWS] = packl[n, :, 0:ROWS]
    h_relay(0)
    relay_block(QKV0, lambda: send_block(UP0))
    h_local.wait()
    for table in tables:
        table.wait()
    h_ready(0)
    block_ready(QKV0)
    attend_all(0, 0)
    for s in range(4):
        d2d(QKV0, s).wait_send()
    for device in (peer(1), peer(2), peer(3), partner):
        pl.semaphore_signal(free, inc=1, device_id={"fsdp": device}, device_id_type=MESH)
    pl.semaphore_wait(free, 4)
    own_block(QKV1)
    own_block(UP1)
    relay_block(UP0, lambda: send_block(QKV1))
    block_ready(UP0)
    own_ready(0)
    mlp_all(0)
    rs_pass_on(0)
    send_block(UP1, (3,))
    relay_block(QKV1)
    block_ready(QKV1)
    h_sent(0)
    residual(0)
    h_send(1)
    qkv_sent()
    own_rows(1)
    attention(1, 0)
    h_relay(1)
    send_block(UP1, (1, 2))
    h_ready(1)
    attend_all(1, 1)

    def rest_of_kv():
        kv_send(0, (1,))
        kv_send(1)

    relay_block(UP1, rest_of_kv)
    block_ready(UP1)
    own_ready(1)
    for n in range(6):
        rs_copy(0, n).wait_send()
    mlp_all(1)
    rs_pass_on(1)
    h_sent(1)
    residual(1)

    for kind in range(5):
        for s in range(4):
            if kind not in (QKV0, QKV1):
                if s > 0:
                    ici(kind, s).wait_send()
                d2d(kind, s).wait_send()
            elif kind == QKV1 and s > 0:
                d2d(kind, s).wait_send()
    for layer in range(2):
        for which in range(2):
            own_remote(layer, which, core).wait_send()
    for n in range(6):
        rs_copy(1, n).wait_send()
    kv_sent(0)
    kv_sent(1)
    for layer in range(2):
        for which in range(2):
            for s in (3, 1, 2):
                kv_copy_in(layer, which, s).wait_recv()


def copy_out(h_in, k_in, v_in, h_out, k_out, v_out, sem):
    pairs = ((h_in, h_out), (k_in, k_out), (v_in, v_out))
    writes = [pltpu.make_async_copy(src, dst, sem.at[n]) for n, (src, dst) in enumerate(pairs)]
    for write in writes:
        write.start()
    for write in writes:
        write.wait()


def rope_tables():
    half = HD // 2
    inv_freq = np.float32(ROPE_BASE) ** (np.float32(-2.0) * np.arange(half, dtype=np.float32) / np.float32(HD))
    angles = np.arange(T, dtype=np.float32)[:, None] * inv_freq.astype(np.float32)[None, :]
    return np.cos(angles).astype(np.float32), np.sin(angles).astype(np.float32)


def solution(mesh):
    batch_spec = P(("dp", "fsdp"))
    weight_spec = P(None, "fsdp")
    cache_spec = P(None, ("dp", "fsdp"))
    vmem = pl.BlockSpec(memory_space=pltpu.VMEM)
    hbm = pl.BlockSpec(memory_space=pl.ANY)
    dma = pltpu.SemaphoreType.DMA

    def per_device(hidden_in, lengths, ln_attn_g, ln_attn_b, ln_mlp_g, ln_mlp_b, w_qkv, w_out, w_up, w_down):
        cos, sin = rope_tables()
        call = pl.pallas_call(
            kernel,
            out_shape=(
                pltpu.VMEM((T, D), BF16),
                pltpu.VMEM((2, 4, T, HD), BF16),
                pltpu.VMEM((2, 4, T, HD), BF16),
            ),
            in_specs=[pl.BlockSpec(memory_space=pltpu.SMEM)] + [hbm] * 11,
            out_specs=(vmem, vmem, vmem),
            scratch_shapes=[
                pltpu.VMEM((4, 2, ROWS), F32),
                pltpu.VMEM((T, HD // 2), F32),
                pltpu.VMEM((T, HD // 2), F32),
                pltpu.VMEM((8, PW), F32),
                pltpu.VMEM((8, 8, PW), F32),
                pltpu.VMEM((2, RAW, 4, 4, HD), BF16),
                pltpu.VMEM((8, D), F32),
                pltpu.VMEM((D, QC), BF16),
                pltpu.VMEM((2, D, FC), BF16),
                pltpu.VMEM((2, 2 * ROWS, D), BF16),
                pltpu.VMEM((2, 2 * DR, D), BF16),
                pltpu.VMEM((5, T, D), BF16),
                pltpu.VMEM((4, 2, T, HALF), F32),
                pltpu.VMEM((2, T, HALF), F32),
                pltpu.VMEM((4, T, HALF), F32),
                pltpu.VMEM((T, D), BF16),
                pltpu.VMEM((T, QC), BF16),
                pltpu.VMEM((4, T, 2 * HD), BF16),
                pltpu.VMEM((2, 4, T, HD), BF16),
                pltpu.VMEM((2, 4, T, HD), BF16),
                dma((5, 4)), dma((5, 4)), dma((5, 4)), dma((5, 4)), dma((5,)),
                dma((2, 2)), dma((2, 2)), dma((2, 2)),
                dma((2,)), dma((2, 3, 2)), dma((2, 3, 2)), dma((2, 2)), dma((2, 2)), dma((1,)),
                dma((2, 6)), dma((2, 6)),
                dma((2, 2, 4)), dma((2, 2, 4)), dma((2, 2)), dma((2,)),
                dma((5,)),
                pltpu.SemaphoreType.REGULAR,
            ],
            compiler_params=pltpu.CompilerParams(
                collective_id=0, has_side_effects=True, vmem_limit_bytes=64500000),
            name="decoder_layers",
        )
        results = call(lengths, ln_attn_g, ln_attn_b, ln_mlp_g, ln_mlp_b, hidden_in[0], w_qkv, w_out, w_up, w_down, cos, sin)
        h_out, kc, vc = pl.pallas_call(
            copy_out,
            out_shape=tuple(jax.ShapeDtypeStruct(r.shape, r.dtype) for r in results),
            in_specs=[hbm] * 3,
            out_specs=(hbm,) * 3,
            scratch_shapes=[dma((3,))],
            compiler_params=pltpu.CompilerParams(vmem_limit_bytes=1 << 20),
            name="copy_out",
        )(*results)
        return h_out[None], kc[:, None], vc[:, None]

    return jax.shard_map(per_device, mesh=mesh, in_specs=(batch_spec, batch_spec) + (weight_spec,) * 8, out_specs=(batch_spec, cache_spec, cache_spec), check_vma=False)
```

```python
import jax
import jax.numpy as jnp
import numpy as np
from jax import lax
from jax.experimental import pallas as pl
from jax.experimental.pallas import tpu as pltpu
from jax.sharding import PartitionSpec as P

MESH = pl.DeviceIdType.MESH
LN_EPS = 1e-5
ROPE_BASE = 10000.0
T = 192
D = 2048
HD = 256
ROWS = 256
QC = 1024
FC = 2048
DR = 1024
HALF = D // 2
UNROLL = 2
PW = ROWS + 128
RAW = 32
CH = 16
TN = 256
F32 = jnp.float32
BF16 = jnp.bfloat16
PACK, QKV0, UP0, QKV1, UP1 = range(5)


def kernel(len_ref, ga_hbm, ba_hbm, gm_hbm, bm_hbm, h_in, wqkv, wout, wup, wdown, cos_hbm, sin_hbm,
           h_out, kc, vc,
           vectors, cos_ref, sin_ref, pack, packl, raw, packg, wq, wu, wo, wd, hg, part, rsd, rsb, nb, qkv, ctx, kr, vr,
           ici_s, ici_r, d2d_s, d2d_r, loc, own_s, own_r, own_l,
           raw_l, h_s, h_r, hf_s, hf_r, h_l, rs_s, rs_r, kv_s, kv_r, kv_l, const_l, small_l, free):
    me = lax.axis_index("fsdp")
    core = me % 2
    chip = me // 2
    partner = chip * 2 + (1 - core)

    def chip_at(s):
        return ((chip // 2 + s // 2) % 2) * 2 + (chip % 2 + s % 2) % 2

    def peer(s):
        return chip_at(s) * 2 + core

    def remote(src, dst, send, recv, device):
        return pltpu.make_async_remote_copy(
            src_ref=src, dst_ref=dst, send_sem=send, recv_sem=recv,
            device_id={"fsdp": device}, device_id_type=MESH)

    def cols(c, width):
        return pl.ds(pl.multiple_of(c * width, width), width)

    def source(kind, c):
        if kind == PACK:
            return pack
        if kind in (QKV0, QKV1):
            return wd.at[1, pl.ds(pl.multiple_of(core * DR + int(kind == QKV1) * 2 * ROWS + (c // 2) * ROWS, ROWS), ROWS), cols(c % 2, QC)]
        return wup.at[int(kind == UP1), :, cols(c, FC)]

    def landing(kind, row):
        if kind == PACK:
            return packl.at[row]
        if kind in (QKV0, QKV1):
            return wq.at[cols(row, ROWS), :]
        return wu.at[int(kind == UP1), cols(row, ROWS), :]

    def ici(kind, s):
        return remote(source(kind, chip_at(s)), landing(kind, me), ici_s.at[kind, s], ici_r.at[kind, s], peer(s))

    def ici_in(kind, s):
        return remote(source(kind, chip), landing(kind, peer(s)), ici_s.at[kind, s], ici_r.at[kind, s], peer(s))

    def d2d(kind, s):
        src = source(kind, chip) if s == 0 else landing(kind, peer(s))
        row = me if s == 0 else peer(s)
        return remote(src, landing(kind, row), d2d_s.at[kind, s], d2d_r.at[kind, s], partner)

    def d2d_in(kind, s):
        row = chip_at(s) * 2 + (1 - core)
        return remote(landing(kind, row), landing(kind, row), d2d_s.at[kind, s], d2d_r.at[kind, s], partner)

    def local(kind):
        return pltpu.make_async_copy(source(kind, chip), landing(kind, me), loc.at[kind])

    def own_refs(layer, which, core_index):
        if which == 0:
            return wout.at[layer], wo.at[layer, cols(core_index, ROWS), :]
        return wdown.at[layer], wd.at[layer, cols(core_index, DR), :]

    def own_remote(layer, which, core_index):
        src, dst = own_refs(layer, which, core_index)
        return remote(src, dst, own_s.at[layer, which], own_r.at[layer, which], partner)

    def own_local(layer, which):
        src, dst = own_refs(layer, which, core)
        return pltpu.make_async_copy(src, dst, own_l.at[layer, which])

    def raw_copy(layer, n, slot):
        return pltpu.make_async_copy(wqkv.at[layer, pl.ds(n * RAW, RAW)], raw.at[slot], raw_l.at[slot])

    def flatten_qkv(layer):
        raw_copy(layer, 0, 0).start()

        def step(n, carry):
            slot = n % 2

            @pl.when(n + 1 < ROWS // RAW)
            def _():
                raw_copy(layer, n + 1, 1 - slot).start()

            raw_copy(layer, n, slot).wait()
            for group in range(4):
                first = core * DR + layer * 2 * ROWS + (group // 2) * ROWS
                rows = pl.ds(pl.multiple_of(first + n * RAW, RAW), RAW)
                for part_of in range(4):
                    at = (group % 2) * QC + part_of * HD
                    wd[1, rows, at:at + HD] = raw[slot, :, group, part_of, :]
            return carry

        lax.fori_loop(0, ROWS // RAW, step, 0)

    def send_block(kind, peers=(3, 1, 2)):
        for s in peers:
            ici(kind, s).start()

    def own_block(kind):
        local(kind).start()
        d2d(kind, 0).start()

    def own_rows(layer):
        for which in range(2):
            own_local(layer, which).start()
            own_remote(layer, which, core).start()

    def relay_block(kind, then=None):
        for n, s in enumerate((3, 1, 2)):
            ici_in(kind, s).wait_recv()
            d2d(kind, s).start()
            if then is not None and n == 0:
                then()

    def block_ready(kind):
        local(kind).wait()
        for s in range(4):
            d2d_in(kind, s).wait_recv()

    def own_ready(layer):
        for which in range(2):
            own_local(layer, which).wait()
            own_remote(layer, which, 1 - core).wait_recv()

    def h_half(j, half):
        return hg.at[j, :, cols(half, HALF)]

    def h_copy(layer, s, half):
        src = h_in.at[:, cols(half, HALF)] if layer == 0 else h_half(chip, half)
        return remote(src, h_half(chip, half), h_s.at[layer, s, half], h_r.at[layer, s, half], peer(s))

    def h_copy_in(layer, s, half):
        dst = h_half(chip_at(s), half)
        return remote(dst, dst, h_s.at[layer, s, half], h_r.at[layer, s, half], peer(s))

    def h_forward(layer, half):
        dst = h_half(chip_at(1 + half), half)
        return remote(dst, dst, hf_s.at[layer, half], hf_r.at[layer, half], peer(2 - half))

    def h_forward_in(layer, half):
        dst = h_half(chip_at(3), half)
        return remote(dst, dst, hf_s.at[layer, half], hf_r.at[layer, half], peer(2 - half))

    def h_send(layer):
        for s, half in ((1, 0), (2, 1), (1, 1), (2, 0)):
            h_copy(layer, s, half).start()

    def h_relay(layer):
        for half in range(2):
            h_copy_in(layer, 1 + half, half).wait_recv()
            h_forward(layer, half).start()

    def h_forwarded(layer):
        for half in range(2):
            h_forward(layer, half).wait_send()

    def h_ready(layer):
        h_forwarded(layer)
        for half in range(2):
            h_copy_in(layer, 2 - half, half).wait_recv()
        for half in range(2):
            h_forward_in(layer, half).wait_recv()

    def h_sent(layer):
        for half in range(2):
            for s in (1, 2):
                h_copy(layer, s, half).wait_send()

    def rs_copy(layer, n):
        s, half, to, dst = (
            (3, 0, 1, rsd.at[0]), (3, 1, 2, rsd.at[1]),
            (1, 0, 1, rsb.at[0]), (2, 1, 2, rsb.at[1]),
            (2, 0, 2, rsb.at[2]), (1, 1, 1, rsb.at[3]))[n]
        return remote(part.at[chip_at(s), half], dst, rs_s.at[layer, n], rs_r.at[layer, n], peer(to))

    def rs_pass_on(layer):
        for half in range(2):
            s = 2 - half
            rs_copy(layer, half).wait_recv()

            def step(i, carry):
                rows = pl.ds(pl.multiple_of(i * CH, CH), CH)
                part[chip_at(s), half, rows, :] = part[chip_at(s), half, rows, :] + rsd[half, rows, :]
                return carry

            lax.fori_loop(0, T // CH, step, 0)
            rs_copy(layer, 4 + half).start()

    def kv_copy(layer, which, s):
        src = (kr, vr)[which].at[layer, chip_at(s)]
        dst = (kc, vc)[which].at[layer, chip]
        return remote(src, dst, kv_s.at[layer, which, s], kv_r.at[layer, which, s], peer(s))

    def kv_copy_in(layer, which, s):
        dst = (kc, vc)[which].at[layer, chip_at(s)]
        return remote(dst, dst, kv_s.at[layer, which, s], kv_r.at[layer, which, s], peer(s))

    def kv_send(layer, parts=(0, 1)):
        for which in parts:
            (kc, vc)[which][layer, chip] = (kr, vr)[which][layer, chip]
            for s in (3, 1, 2):
                kv_copy(layer, which, s).start()

    def kv_sent(layer):
        for which in range(2):
            for s in (3, 1, 2):
                kv_copy(layer, which, s).wait_send()

    def hm_slot(s):
        own = 1 - (s + 3) // 4
        return own * 4 + (1 - own) * chip_at(s)

    def norm(layer, s):
        gain_a, bias_a, gain_m, bias_m = (packg[2 * n + layer:2 * n + layer + 1, :] for n in range(4))

        def step(i, carry):
            rows = pl.ds(pl.multiple_of(i * CH, CH), CH)
            x = hg[chip_at(s), rows, :].astype(F32)
            mean = jnp.sum(x, axis=-1, keepdims=True) * (1.0 / D)
            x = x - mean
            var = jnp.sum(x * x, axis=-1, keepdims=True) * (1.0 / D)
            x = x * lax.rsqrt(var + LN_EPS)
            nb[rows, :] = (x * gain_a + bias_a).astype(BF16)
            hg[hm_slot(s), rows, :] = (x * gain_m + bias_m).astype(BF16)
            return carry

        lax.fori_loop(0, T // CH, step, 0, unroll=UNROLL)

    def rope(u):
        u = u.astype(F32)
        lo, hi = u[:, :HD // 2], u[:, HD // 2:]
        cos, sin = cos_ref[...], sin_ref[...]
        return jnp.concatenate([lo * cos - hi * sin, hi * cos + lo * sin], axis=-1).astype(BF16)

    def attention(layer, s):
        j = chip_at(s)
        norm(layer, s)

        def project(i, carry):
            n = cols(i, TN)
            qkv[:, n] = jnp.dot(nb[...], wq[:, n], preferred_element_type=F32).astype(BF16)
            return carry

        lax.fori_loop(0, QC // TN, project, 0)
        key = rope(qkv[:, 2 * HD:3 * HD])
        kr[layer, j] = key
        vr[layer, j] = qkv[:, 3 * HD:4 * HD]
        length = packl[j * 2 + core, 0:1, ROWS:PW][:, 0:1]
        query_pos = lax.broadcasted_iota(jnp.int32, (T, T), 0)
        key_pos = lax.broadcasted_iota(jnp.int32, (T, T), 1)
        allowed = (key_pos <= query_pos) & (key_pos.astype(F32) < length)
        for head in range(2):
            query = rope(qkv[:, head * HD:(head + 1) * HD])
            scores = lax.dot_general(query, key, (((1,), (1,)), ((), ())), preferred_element_type=F32) * (HD ** -0.5)
            scores = jnp.where(allowed, scores, -1e30)
            expo = jnp.exp(scores - jnp.max(scores, axis=-1, keepdims=True))
            prob = (expo / jnp.sum(expo, axis=-1, keepdims=True)).astype(BF16)
            ctx[j, :, head * HD:(head + 1) * HD] = jnp.dot(prob, vr[layer, j], preferred_element_type=F32).astype(BF16)

    def mlp(layer, s):
        j = chip_at(s)
        hm = hg.at[hm_slot(s)]

        def up(i, carry):
            n = cols(i, TN)
            u = jnp.dot(hm[...], wu[layer, :, n], preferred_element_type=F32)
            nb[:, n] = (0.5 * u * (1.0 + lax.erf(u * np.float32(np.sqrt(0.5))))).astype(BF16)
            return carry

        lax.fori_loop(0, FC // TN, up, 0)

        def down(i, carry):
            n = cols(i, TN)
            acc = jnp.dot(nb[...], wd[layer, :, n], preferred_element_type=F32)
            acc = acc + jnp.dot(ctx[j], wo[layer, :, n], preferred_element_type=F32)
            part[j, i // (HALF // TN), :, cols(i % (HALF // TN), TN)] = acc
            return carry

        for half, sends in ((0, ((0, 3), (2, 1))), (1, ((1, 3), (3, 2)))):
            lax.fori_loop(half * (HALF // TN), (half + 1) * (HALF // TN), down, 0)
            for n, at in sends:
                @pl.when(s == at)
                def _():
                    rs_copy(layer, n).start()

    def residual(layer):
        for half in range(2):
            rs_copy(layer, 2 + half).wait_recv()
        if layer == 0:
            kv_send(0, (0,))

        def direct(i, carry):
            rows = pl.ds(pl.multiple_of(i * CH, CH), CH)
            for half in range(2):
                total = hg[chip, rows, cols(half, HALF)].astype(F32) + part[chip, half, rows, :]
                part[chip, half, rows, :] = total + rsb[half, rows, :]
            return carry

        lax.fori_loop(0, T // CH, direct, 0)
        for half in range(2):
            rs_copy(layer, 4 + half).wait_recv()

        def step(i, carry):
            rows = pl.ds(pl.multiple_of(i * CH, CH), CH)
            for half in range(2):
                total = (part[chip, half, rows, :] + rsb[2 + half, rows, :]).astype(BF16)
                if layer == 0:
                    hg[chip, rows, cols(half, HALF)] = total
                else:
                    h_out[rows, half * HALF:(half + 1) * HALF] = total
            return carry

        lax.fori_loop(0, T // CH, step, 0)

    def qkv_sent():
        for kind in (QKV0, QKV1):
            for s in (3, 1, 2):
                ici(kind, s).wait_send()
        d2d(QKV1, 0).wait_send()

    def attend_all(layer, first):
        def step(s, carry):
            attention(layer, s)
            return carry

        lax.fori_loop(first, 4, step, 0)

    def mlp_all(layer):
        def step(i, carry):
            mlp(layer, 3 - i)
            return carry

        lax.fori_loop(0, 4, step, 0)

    small = [pltpu.make_async_copy(src, vectors.at[n], small_l.at[n])
             for n, src in enumerate((ga_hbm, ba_hbm, gm_hbm, bm_hbm))]
    for copy in small:
        copy.start()
    barrier = pltpu.get_barrier_semaphore()
    for s in (1, 2, 3):
        pl.semaphore_signal(barrier, inc=1, device_id={"fsdp": peer(s)}, device_id_type=MESH)
    pl.semaphore_signal(barrier, inc=1, device_id={"fsdp": partner}, device_id_type=MESH)
    pl.semaphore_wait(barrier, 4)

    h_send(0)
    h_local = pltpu.make_async_copy(h_in, hg.at[chip], h_l.at[0])
    h_local.start()
    tables = [pltpu.make_async_copy(src, dst, const_l.at[n])
              for n, (src, dst) in enumerate(((cos_hbm, cos_ref), (sin_hbm, sin_ref)))]
    for table in tables:
        table.start()
    for copy in small:
        copy.wait()
    for n in range(4):
        pack[2 * n:2 * n + 2, 0:ROWS] = vectors[n]
    pack[:, ROWS:PW] = jnp.full((8, PW - ROWS), len_ref[0].astype(F32), F32)
    flatten_qkv(0)
    send_block(PACK)
    own_block(PACK)
    send_block(QKV0)
    own_block(QKV0)
    own_block(UP0)
    own_rows(0)
    flatten_qkv(1)
    relay_block(PACK)
    block_ready(PACK)
    for n in range(8):
        packg[:, n * ROWS:(n + 1) * ROWS] = packl[n, :, 0:ROWS]
    h_relay(0)
    relay_block(QKV0, lambda: send_block(UP0))
    h_local.wait()
    for table in tables:
        table.wait()
    h_ready(0)
    block_ready(QKV0)
    attend_all(0, 0)
    for s in range(4):
        d2d(QKV0, s).wait_send()
    for device in (peer(1), peer(2), peer(3), partner):
        pl.semaphore_signal(free, inc=1, device_id={"fsdp": device}, device_id_type=MESH)
    pl.semaphore_wait(free, 4)
    send_block(QKV1)
    own_block(QKV1)
    own_block(UP1)
    relay_block(UP0)
    block_ready(UP0)
    own_ready(0)
    mlp_all(0)
    rs_pass_on(0)
    send_block(UP1, (3,))
    relay_block(QKV1)
    block_ready(QKV1)
    h_sent(0)
    residual(0)
    h_send(1)
    qkv_sent()
    own_rows(1)
    attention(1, 0)
    h_relay(1)
    send_block(UP1, (1, 2))
    h_ready(1)
    attend_all(1, 1)

    def rest_of_kv():
        kv_send(0, (1,))
        kv_send(1)

    relay_block(UP1, rest_of_kv)
    block_ready(UP1)
    own_ready(1)
    for n in range(6):
        rs_copy(0, n).wait_send()
    mlp_all(1)
    rs_pass_on(1)
    h_sent(1)
    residual(1)

    for kind in range(5):
        for s in range(4):
            if kind not in (QKV0, QKV1):
                if s > 0:
                    ici(kind, s).wait_send()
                d2d(kind, s).wait_send()
            elif kind == QKV1 and s > 0:
                d2d(kind, s).wait_send()
    for layer in range(2):
        for which in range(2):
            own_remote(layer, which, core).wait_send()
    for n in range(6):
        rs_copy(1, n).wait_send()
    kv_sent(0)
    kv_sent(1)
    for layer in range(2):
        for which in range(2):
            for s in (3, 1, 2):
                kv_copy_in(layer, which, s).wait_recv()


def copy_out(h_in, k_in, v_in, h_out, k_out, v_out, sem):
    pairs = ((h_in, h_out), (k_in, k_out), (v_in, v_out))
    writes = [pltpu.make_async_copy(src, dst, sem.at[n]) for n, (src, dst) in enumerate(pairs)]
    for write in writes:
        write.start()
    for write in writes:
        write.wait()


def rope_tables():
    half = HD // 2
    inv_freq = np.float32(ROPE_BASE) ** (np.float32(-2.0) * np.arange(half, dtype=np.float32) / np.float32(HD))
    angles = np.arange(T, dtype=np.float32)[:, None] * inv_freq.astype(np.float32)[None, :]
    return np.cos(angles).astype(np.float32), np.sin(angles).astype(np.float32)


def solution(mesh):
    batch_spec = P(("dp", "fsdp"))
    weight_spec = P(None, "fsdp")
    cache_spec = P(None, ("dp", "fsdp"))
    vmem = pl.BlockSpec(memory_space=pltpu.VMEM)
    hbm = pl.BlockSpec(memory_space=pl.ANY)
    dma = pltpu.SemaphoreType.DMA

    def per_device(hidden_in, lengths, ln_attn_g, ln_attn_b, ln_mlp_g, ln_mlp_b, w_qkv, w_out, w_up, w_down):
        cos, sin = rope_tables()
        call = pl.pallas_call(
            kernel,
            out_shape=(
                pltpu.VMEM((T, D), BF16),
                pltpu.VMEM((2, 4, T, HD), BF16),
                pltpu.VMEM((2, 4, T, HD), BF16),
            ),
            in_specs=[pl.BlockSpec(memory_space=pltpu.SMEM)] + [hbm] * 11,
            out_specs=(vmem, vmem, vmem),
            scratch_shapes=[
                pltpu.VMEM((4, 2, ROWS), F32),
                pltpu.VMEM((T, HD // 2), F32),
                pltpu.VMEM((T, HD // 2), F32),
                pltpu.VMEM((8, PW), F32),
                pltpu.VMEM((8, 8, PW), F32),
                pltpu.VMEM((2, RAW, 4, 4, HD), BF16),
                pltpu.VMEM((8, D), F32),
                pltpu.VMEM((D, QC), BF16),
                pltpu.VMEM((2, D, FC), BF16),
                pltpu.VMEM((2, 2 * ROWS, D), BF16),
                pltpu.VMEM((2, 2 * DR, D), BF16),
                pltpu.VMEM((5, T, D), BF16),
                pltpu.VMEM((4, 2, T, HALF), F32),
                pltpu.VMEM((2, T, HALF), F32),
                pltpu.VMEM((4, T, HALF), F32),
                pltpu.VMEM((T, D), BF16),
                pltpu.VMEM((T, QC), BF16),
                pltpu.VMEM((4, T, 2 * HD), BF16),
                pltpu.VMEM((2, 4, T, HD), BF16),
                pltpu.VMEM((2, 4, T, HD), BF16),
                dma((5, 4)), dma((5, 4)), dma((5, 4)), dma((5, 4)), dma((5,)),
                dma((2, 2)), dma((2, 2)), dma((2, 2)),
                dma((2,)), dma((2, 3, 2)), dma((2, 3, 2)), dma((2, 2)), dma((2, 2)), dma((1,)),
                dma((2, 6)), dma((2, 6)),
                dma((2, 2, 4)), dma((2, 2, 4)), dma((2, 2)), dma((2,)),
                dma((5,)),
                pltpu.SemaphoreType.REGULAR,
            ],
            compiler_params=pltpu.CompilerParams(
                collective_id=0, has_side_effects=True, vmem_limit_bytes=64500000),
            name="decoder_layers",
        )
        results = call(lengths, ln_attn_g, ln_attn_b, ln_mlp_g, ln_mlp_b, hidden_in[0], w_qkv, w_out, w_up, w_down, cos, sin)
        h_out, kc, vc = pl.pallas_call(
            copy_out,
            out_shape=tuple(jax.ShapeDtypeStruct(r.shape, r.dtype) for r in results),
            in_specs=[hbm] * 3,
            out_specs=(hbm,) * 3,
            scratch_shapes=[dma((3,))],
            compiler_params=pltpu.CompilerParams(vmem_limit_bytes=1 << 20),
            name="copy_out",
        )(*results)
        return h_out[None], kc[:, None], vc[:, None]

    return jax.shard_map(per_device, mesh=mesh, in_specs=(batch_spec, batch_spec) + (weight_spec,) * 8, out_specs=(batch_spec, cache_spec, cache_spec), check_vma=False)
```
